32 devices in a mesh: tm: 4 (over z), par: 8 (over y, x, core).
Axes of the slice: x: 2, y: 2, z: 4, core: 2. Of those that a mesh axis runs over, the one named last changes fastest.
Arguments:
- kernel: bfloat16 [64, 256, 1024], P('tm', None, 'par'), may hold values from -0.03125 to 0.03125
- history: bfloat16 [64, 1024, 128], P('tm', 'par'), may hold values from -6 to 6
- arrivals: bfloat16 [2, 16, 1024, 128], P(None, 'tm', 'par'), may hold values from -6 to 6
Outputs:
- observations: bfloat16 [2, 16, 256, 128], P(None, None, ('tm', 'par'))
The draws below stay inside these ranges and needn't reach their ends.
All inputs are finite; a program needn't handle non-finite values.
Results may differ from the reference program's by a relative error of at most 0.014.
Values may be sent and summed in bfloat16 or wider, within the bound.
A program may use at most 64 MiB of HBM per device.

```python
import jax
import jax.numpy as jnp
from jax import lax

TB = 16
NF = 17
SENS = 256
FIELDS = 128
STEPS = 2
NT = 64
NP = 1024
N_TM = 4


def strengthened(entries, stream_key, source, target, shards_of, factor):
    owner, partner = [(jnp.arange(entries.shape[axis_at]) // (entries.shape[axis_at] // shards_of)).reshape([-1 if axis == axis_at else 1 for axis in range(entries.ndim)]) for axis_at in (source, target)]
    chosen = jax.random.permutation(stream_key, shards_of)[partner]
    strong = (owner == chosen) | (owner == (partner + shards_of // 2) % shards_of)
    return jnp.where(strong, factor * entries, entries)


def levels(own_key, dims, cuts, least, top_value):
    def one(position, parts):
        draws = jax.random.uniform(jax.random.fold_in(jax.random.fold_in(own_key, 6), position), (parts,), jnp.float32, least / len(cuts), top_value / len(cuts))
        return jnp.repeat(jnp.exp(draws), dims[position] // parts).reshape((-1,) + (1,) * (len(dims) - position - 1))

    gain = one(*cuts[0])
    for cut in cuts[1:]:
        gain = gain * one(*cut)
    return gain


def normal_values(rng, shape, scale, limit, cuts=(), kind=jnp.bfloat16):
    loudness = levels(rng, shape, cuts, -0.22, 0.18) if cuts else 1.0
    result = jax.random.normal(rng, shape, jnp.float32) * scale * loudness
    return jnp.minimum(jnp.maximum(result, -limit), limit).astype(kind)


def noise_with(key, shape, spread, reach, shards, heavy, kind=jnp.bfloat16):
    drawn = spread * jax.random.normal(key, shape, jnp.float32)
    if shards:
        drawn = drawn * levels(key, shape, shards, -0.22, 0.18)
    return jnp.clip(strengthened(drawn, jax.random.fold_in(key, 3), *heavy), -reach, reach).astype(kind)


def setup_inputs(seed: int = 0) -> dict:
    streams_of = jax.random.split(jax.random.key(seed), 4)
    return {
        "kernel": noise_with(streams_of[0], (NT, SENS, NP), (NT * NP) ** -0.5, 0.03125, ((0, 4), (2, 8)), (2, 1, 8, 2.0)),
        "history": normal_values(streams_of[1], (NT, NP, FIELDS), 1.0, 6.0, ((0, 4), (1, 8))),
        "arrivals": normal_values(streams_of[2], (STEPS, TB, NP, FIELDS), 1.0, 6.0, ((1, 4), (2, 8))),
    }


def rounded(values):
    narrow = values.astype(jnp.bfloat16)
    narrow = lax.optimization_barrier(narrow)
    return narrow.astype(jnp.float32)


def reference(kernel, history, arrivals):
    length = 2 * TB
    ordered = jnp.concatenate([history.reshape(N_TM, TB, NP, FIELDS)[::-1], arrivals], 0)
    accum_shape = (STEPS, NF, SENS, FIELDS)

    def one_lag(totals, lag_index):
        real_acc, imag_acc = totals
        first_row = (lag_index * TB).astype(jnp.int32)
        lag_block = lax.dynamic_slice_in_dim(kernel, first_row, TB, 0).astype(jnp.float32)
        spectrum = jnp.fft.rfft(lag_block, n=length, axis=0)
        kernel_real_component = rounded(jnp.real(spectrum))
        kernel_imaginary = rounded(jnp.imag(spectrum))
        for step_index in range(STEPS):
            first_block = (N_TM - 1 + step_index - lag_index).astype(jnp.int32)
            window = lax.dynamic_slice_in_dim(ordered, first_block, 2, 0)
            window = window.reshape(length, NP, FIELDS).astype(jnp.float32)
            window_spec = jnp.fft.rfft(window, axis=0)
            window_real_component = rounded(jnp.real(window_spec))
            window_imaginary = rounded(jnp.imag(window_spec))
            real_component = jnp.einsum("njy,nyv->njv", kernel_real_component, window_real_component, precision=lax.Precision.HIGHEST)
            real_component = real_component - jnp.einsum("njy,nyv->njv", kernel_imaginary, window_imaginary, precision=lax.Precision.HIGHEST)
            imaginary_component = jnp.einsum("njy,nyv->njv", kernel_real_component, window_imaginary, precision=lax.Precision.HIGHEST)
            imaginary_component = imaginary_component + jnp.einsum("njy,nyv->njv", kernel_imaginary, window_real_component, precision=lax.Precision.HIGHEST)
            real_acc = real_acc.at[step_index].add(real_component)
            imag_acc = imag_acc.at[step_index].add(imaginary_component)
        return (real_acc, imag_acc), None

    zeros_start = jnp.zeros(accum_shape, jnp.float32)
    (real_acc, imag_acc), unused = lax.scan(one_lag, (zeros_start, zeros_start), jnp.arange(N_TM, dtype=jnp.int32))
    signal = jnp.fft.irfft(lax.complex(real_acc, imag_acc), n=length, axis=1)
    return signal[:, TB:].astype(jnp.bfloat16)
```

```python
import functools

import jax
import jax.numpy as jnp
from jax import lax
from jax.experimental import pallas as pl
from jax.experimental.pallas import tpu as pltpu
from jax.sharding import PartitionSpec as P

MESH = pl.DeviceIdType.MESH
F32 = jnp.float32
VMEM_BYTES = 67_043_328
SPLIT = 1
PIECE_US, CORE_US, CHIP_US, TM_US, HOLD_US, FINISH_US = 2.8, 1.5, 3.0, 4.0, 9.0, 8.0


def kernel_body(
    tm_count, group, split, k_ref, h_ref, a_ref, out_ref, kflat, xbuf, buf0, rcv0, mid, mrcv,
    zbuf, zrcv, load_s, hist_s, fwd_s, arr_s, x_r, s0, r0, ms, mr, zs, zr
):
    block_len, sensors, params = k_ref.shape
    fields = xbuf.shape[2]
    steps = out_ref.shape[0]
    piece = block_len // tm_count
    sub = piece // split
    block_chunks = tm_count * split
    chunks = steps * block_chunks
    rows = sensors // (tm_count * group * 2)
    k = lax.axis_index("tm")
    par = lax.axis_index("par")
    core, chip = par % 2, par // 2
    partner = par + 1 - 2 * core
    flips = sorted(range(1, group), key=lambda flip: -flip.bit_count())

    def flipped(flip):
        target = chip
        for b in range(flip.bit_length()):
            if flip >> b & 1:
                target = target + (1 - 2 * ((chip // (1 << b)) % 2)) * (1 << b)
        return target

    order = [
        (tm * group + q) * 2 + half
        for half in range(2)
        for q in range(group)
        for tm in range(tm_count)
    ]

    loads = [pltpu.make_async_copy(h_ref, xbuf.at[pl.ds(0, block_len)], load_s.at[block_len])]
    for j in range(block_len):
        loads.append(
            pltpu.make_async_copy(
                k_ref.at[block_len - 1 - j],
                kflat.at[:, pl.ds(j * params, params)],
                load_s.at[j],
            )
        )
    first_pieces = []
    for s in range(steps):
        place = xbuf.at[pl.ds(block_len * (s + 1), piece)]
        first_pieces.append(
            pltpu.make_async_copy(a_ref.at[s], place, load_s.at[block_len + 1 + s])
        )
    place = xbuf.at[pl.ds(2 * block_len + piece, piece)]
    own_piece = pltpu.make_async_copy(a_ref.at[0], place, load_s.at[block_len + 1])

    barrier = pltpu.get_barrier_semaphore()
    for d in range(1, tm_count):
        pl.semaphore_signal(
            barrier, inc=1, device_id={"tm": lax.rem(k + d, tm_count)}, device_id_type=MESH
        )
    for d in flips:
        peer = flipped(d) * 2 + core
        pl.semaphore_signal(barrier, inc=1, device_id={"par": peer}, device_id_type=MESH)
    pl.semaphore_signal(barrier, inc=1, device_id={"par": partner}, device_id_type=MESH)

    for copy in loads:
        copy.start()

    @pl.when(k == 0)
    def _():
        for copy in first_pieces:
            copy.start()

    pl.when(k == 1)(own_piece.start)

    pl.semaphore_wait(barrier, tm_count + group - 1)

    def remote(src, dst, send, recv, where):
        return pltpu.make_async_remote_copy(
            src_ref=src, dst_ref=dst, send_sem=send, recv_sem=recv, device_id=where,
            device_id_type=MESH,
        )

    def slot(c):
        return xbuf.at[pl.ds(block_len + c * sub, sub)]

    up = {"tm": jnp.minimum(k + 1, tm_count - 1)}

    def arrival_copy(n, s, target, base, part):
        c = (base + k) * split + part
        return remote(
            a_ref.at[s, pl.ds(part * sub, sub)], slot(c), arr_s.at[n, part], x_r.at[c],
            {"tm": target},
        )

    arrival_copies = []
    for n, s, target, base in ((0, 0, 0, 0), (1, 0, 1, tm_count), (2, 1, 0, tm_count)):
        for part in range(split):
            arrival_copies.append((k != target, arrival_copy(n, s, target, base, part)))
    history_copies = [
        remote(xbuf.at[pl.ds(i * sub, sub)], slot(i), hist_s.at[i], x_r.at[i], up)
        for i in range(block_chunks)
    ]
    forward_copies = [
        remote(slot(i), slot(i + block_chunks), fwd_s.at[i], x_r.at[i + block_chunks], up)
        for i in range(block_chunks)
    ]
    sends_up = k < tm_count - 1
    forwards = (k > 0) & (k < tm_count - 1)

    loads[0].wait()

    @pl.when(sends_up)
    def _():
        for copy in history_copies:
            copy.start()

    for condition, copy in arrival_copies:
        pl.when(condition)(copy.start)

    for copy in loads[1:]:
        copy.wait()

    @pl.when(k == 0)
    def _():
        for copy in first_pieces:
            copy.wait()

    pl.when(k == 1)(own_piece.wait)

    def receive(c):
        copy = remote(slot(c), slot(c), hist_s.at[0], x_r.at[c], up)
        source = c // split
        if source % tm_count == 0:
            pl.when(k != 0)(copy.wait_recv)
        elif source == tm_count + 1:
            pl.when(k != 1)(copy.wait_recv)
        else:
            copy.wait_recv()

    def core_copy(c):
        return remote(buf0.at[c, 1 - core], rcv0.at[c], s0.at[c], r0.at[c], {"par": partner})

    def chip_copy(c, d):
        target = flipped(d)
        return remote(
            mid.at[c, target], mrcv.at[c, d - 1], ms.at[c, d - 1], mr.at[c, d - 1],
            {"par": target * 2 + core},
        )

    def tm_copy(c, d):
        target = lax.rem(k + d, tm_count)
        return remote(
            zbuf.at[c, target], zrcv.at[c, d - 1], zs.at[c, d - 1], zr.at[c, d - 1], {"tm": target}
        )

    def compute(c):
        receive(c)
        if c < block_chunks:
            pl.when(forwards)(forward_copies[c].start)
        share = sensors // (2 * group)
        for q in range(sub // 2):
            first = c * sub + 2 * q + 1
            left = xbuf[pl.ds(first, block_len)].reshape(block_len * params, fields)
            right = xbuf[pl.ds(first + 1, block_len)].reshape(block_len * params, fields)
            both = jnp.concatenate([left, right], 1)
            total = jnp.dot(kflat[...], both, preferred_element_type=F32)
            for side in range(2):
                mine = total[:, side * fields : (side + 1) * fields]
                moved = jnp.concatenate([mine[o * rows : (o + 1) * rows] for o in order], 0)
                moved = moved.astype(jnp.bfloat16)
                for n in range(2 * group):
                    part = moved[n * share : (n + 1) * share]
                    buf0[c, n // group, n % group, 2 * q + side] = part
        core_copy(c).start()

    def across(c):
        core_copy(c).wait_recv()
        total = buf0[c, core].astype(F32) + rcv0[c].astype(F32)
        mid[c] = total.astype(jnp.bfloat16)
        for d in flips:
            chip_copy(c, d).start()

    def spread(c):
        total = mid[c, chip].astype(F32)
        for d in range(1, group):
            chip_copy(c, d).wait_recv()
            total = total + mrcv[c, d - 1].astype(F32)
        for t in range(tm_count):
            parts = [total[g, t * rows : (t + 1) * rows] for g in range(sub)]
            zbuf[c, t] = jnp.concatenate(parts, 0).astype(jnp.bfloat16)
        for d in range(1, tm_count):
            tm_copy(c, d).start()

    def finish(c):
        total = zbuf[c, k].astype(F32)
        for d in range(1, tm_count):
            tm_copy(c, d).wait_recv()
            total = total + zrcv[c, d - 1].astype(F32)
        begin = (c % block_chunks) * sub
        out_ref[c // block_chunks, begin : begin + sub] = total.reshape(sub, rows, fields).astype(
            out_ref.dtype
        )

    stages = (compute, across, spread, finish)
    waits = (0.0, CORE_US, CHIP_US, TM_US)
    interval = PIECE_US / split
    events = []
    for c in range(chunks):
        time = interval * c
        for lag, stage in enumerate(stages):
            time += waits[lag]
            if stage is spread:
                time = max(time, interval * block_chunks + HOLD_US)
            if stage is finish:
                time = max(time, interval * chunks + FINISH_US)
            events.append((time, -lag, c, stage))
    for _, _, c, stage in sorted(events, key=lambda event: event[:3]):
        stage(c)

    @pl.when(sends_up)
    def _():
        for copy in history_copies:
            copy.wait_send()

    @pl.when(forwards)
    def _():
        for copy in forward_copies:
            copy.wait_send()

    for condition, copy in arrival_copies:
        pl.when(condition)(copy.wait_send)
    for c in range(chunks):
        core_copy(c).wait_send()
        for d in range(1, group):
            chip_copy(c, d).wait_send()
        for d in range(1, tm_count):
            tm_copy(c, d).wait_send()


def fused(tm_count, group, kernel, history, arrivals):
    block_len, sensors, params = kernel.shape
    fields = history.shape[2]
    steps = arrivals.shape[0]
    piece = block_len // tm_count
    split = SPLIT if piece % (2 * SPLIT) == 0 else 1
    sub = piece // split
    chunks = steps * tm_count * split
    share = sensors // (2 * group)
    rows = share // tm_count
    bf16 = jnp.bfloat16
    dma = pltpu.SemaphoreType.DMA
    out_bytes = steps * block_len * rows * fields * 2
    scratch = [
        pltpu.VMEM((sensors, block_len * params), bf16),
        pltpu.VMEM(((steps + 1) * block_len, params, fields), bf16),
        pltpu.VMEM((chunks, 2, group, sub, share, fields), bf16),
        pltpu.VMEM((chunks, group, sub, share, fields), bf16),
        pltpu.VMEM((chunks, group, sub, share, fields), bf16),
        pltpu.VMEM((chunks, group - 1, sub, share, fields), bf16),
        pltpu.VMEM((chunks, tm_count, sub * rows, fields), bf16),
        pltpu.VMEM((chunks, tm_count - 1, sub * rows, fields), bf16),
        dma((block_len + 1 + steps,)),
        dma((tm_count * split,)),
        dma((tm_count * split,)),
        dma((3, split)),
        dma((chunks,)),
        dma((chunks,)),
        dma((chunks,)),
        dma((chunks, group - 1)),
        dma((chunks, group - 1)),
        dma((chunks, tm_count - 1)),
        dma((chunks, tm_count - 1)),
    ]
    return pl.pallas_call(
        functools.partial(kernel_body, tm_count, group, split),
        out_shape=pltpu.VMEM((steps, block_len, rows, fields), bf16),
        in_specs=[pl.BlockSpec(memory_space=pltpu.HBM)] * 3,
        out_specs=pl.BlockSpec(memory_space=pltpu.VMEM),
        scratch_shapes=scratch,
        compiler_params=pltpu.CompilerParams(
            collective_id=0, has_side_effects=True, vmem_limit_bytes=VMEM_BYTES - 2 * out_bytes
        ),
    )(kernel, history, arrivals)


def plain(tm_count, kernel, history, arrivals):
    block_len, sensors, params = kernel.shape
    fields = history.shape[2]
    steps = arrivals.shape[0]
    incoming = lax.all_gather(arrivals, "tm", axis=1, tiled=True)
    position = lax.axis_index("tm")
    pairs = [(i, i + 1) for i in range(tm_count - 1)]
    blocks = [history]
    for s in range(steps):
        shifted = lax.ppermute(blocks[-1], "tm", pairs)
        blocks.append(jnp.where(position == 0, incoming[s], shifted))
    window = jnp.concatenate(blocks, 0)
    flat = kernel[::-1].transpose(1, 0, 2).reshape(sensors, block_len * params)

    def one(first):
        part = lax.dynamic_slice_in_dim(window, first, block_len, 0)
        part = part.reshape(block_len * params, fields)
        return jnp.dot(flat, part, preferred_element_type=F32)

    partial = lax.map(one, jnp.arange(steps * block_len, dtype=jnp.int32) + 1)
    partial = partial.reshape(steps, block_len, sensors, fields)
    total = lax.psum_scatter(partial, ("tm", "par"), scatter_dimension=2, tiled=True)
    return total.astype(jnp.bfloat16)


def solution(mesh):
    tm_count, par_count = mesh.shape["tm"], mesh.shape["par"]

    def per_device(kernel, history, arrivals):
        rows = kernel.shape[1] // (tm_count * par_count)
        piece = kernel.shape[0] // tm_count
        fits = rows % 8 == 0 and piece % 2 == 0 and tm_count > 1 and arrivals.shape[0] == 2
        if fits and par_count > 2 and par_count.bit_count() == 1:
            return fused(tm_count, par_count // 2, kernel, history, arrivals)
        return plain(tm_count, kernel, history, arrivals)

    in_specs = (P("tm", None, "par"), P("tm", "par", None), P(None, "tm", "par", None))
    out_specs = P(None, None, ("tm", "par"), None)
    return jax.shard_map(
        per_device, mesh=mesh, in_specs=in_specs, out_specs=out_specs, check_vma=False
    )
```

```python
import functools

import jax
import jax.numpy as jnp
from jax import lax
from jax.experimental import pallas as pl
from jax.experimental.pallas import tpu as pltpu
from jax.sharding import PartitionSpec as P

MESH = pl.DeviceIdType.MESH
F32 = jnp.float32
BF16 = jnp.bfloat16
VMEM_BYTES = 67_043_328


def kernel_body(
    tm_count, group, k_ref, h_ref, a_ref, out_ref, kflat, kext, xbuf, zext, buf0, rcv0, mid, mrcv,
    zbuf, zrcv, load_s, hist_s, fwd_s, arr_s, relay_s, ext_s, x_r, ext_r, s0, r0, ms, mr, zs, zr,
    ready
):
    block_len, sensors, params = k_ref.shape
    fields = xbuf.shape[2]
    steps = out_ref.shape[0]
    piece = block_len // tm_count
    pieces = steps * tm_count
    last = pieces - 1
    rows = sensors // (tm_count * group * 2)
    share = sensors // (2 * group)
    k = lax.axis_index("tm")
    par = lax.axis_index("par")
    core, chip = par % 2, par // 2
    partner = par + 1 - 2 * core
    flips = sorted(range(1, group), key=lambda flip: -flip.bit_count())
    top = tm_count - 1

    def flipped(flip):
        target = chip
        for b in range(flip.bit_length()):
            if flip >> b & 1:
                target = target + (1 - 2 * ((chip // (1 << b)) % 2)) * (1 << b)
        return target

    order = [
        (tm * group + q) * 2 + half
        for half in range(2)
        for q in range(group)
        for tm in range(tm_count)
    ]

    def remote(src, dst, send, recv, where):
        return pltpu.make_async_remote_copy(
            src_ref=src, dst_ref=dst, send_sem=send, recv_sem=recv, device_id=where,
            device_id_type=MESH,
        )

    def signal(sem, where):
        pl.semaphore_signal(sem, inc=1, device_id=where, device_id_type=MESH)

    barrier = pltpu.get_barrier_semaphore()
    pl.when(k > 0)(lambda: signal(barrier, {"tm": jnp.maximum(k - 1, 0)}))
    for d in flips:
        signal(barrier, {"par": flipped(d) * 2 + core})
    signal(barrier, {"par": partner})

    loads = [pltpu.make_async_copy(h_ref, xbuf.at[pl.ds(0, block_len)], load_s.at[block_len])]
    for j in range(block_len):
        loads.append(
            pltpu.make_async_copy(
                k_ref.at[block_len - 1 - j],
                kflat.at[:, pl.ds(j * params, params)],
                load_s.at[j],
            )
        )
    first_pieces = []
    for s in range(steps):
        place = xbuf.at[pl.ds(block_len * (s + 1), piece)]
        first_pieces.append(
            pltpu.make_async_copy(a_ref.at[s], place, load_s.at[block_len + 1 + s])
        )
    place = xbuf.at[pl.ds(2 * block_len + piece, piece)]
    own_piece = pltpu.make_async_copy(a_ref.at[0], place, load_s.at[block_len + 1])

    for copy in loads:
        copy.start()

    @pl.when(k == 0)
    def _():
        for copy in first_pieces:
            copy.start()

    pl.when(k == 1)(own_piece.start)

    @pl.when((k == 0) | (k == top))
    def _():
        kext[...] = jnp.zeros_like(kext)

    @pl.when(k > 1)
    def _():
        tail = xbuf.at[pl.ds(block_len + last * piece, piece)]
        tail[...] = jnp.zeros(tail.shape, BF16)

    zext[pl.ds(0, piece - 1)] = jnp.zeros((piece - 1, params, fields), BF16)

    pl.semaphore_wait(barrier, group + (k < top).astype(jnp.int32))

    def slot(c):
        return xbuf.at[pl.ds(block_len + c * piece, piece)]

    up, down = {"tm": jnp.minimum(k + 1, top)}, {"tm": jnp.maximum(k - 1, 0)}
    sends_up = k < top
    forwards = (k > 0) & (k < top)
    relays = k == 1

    history_copies = [
        remote(xbuf.at[pl.ds(i * piece, piece)], slot(i), hist_s.at[i], x_r.at[i], up)
        for i in range(tm_count)
    ]
    forward_copies = [
        remote(slot(i), slot(i + tm_count), fwd_s.at[i], x_r.at[i + tm_count], up)
        for i in range(tm_count - 1)
    ]

    def arrival_copy(n, s, target, c):
        return remote(a_ref.at[s], slot(c), arr_s.at[n], x_r.at[c], {"tm": target})

    arrival_copies = [
        (k == 0, arrival_copy(0, 0, 1, tm_count)),
        (k == 1, arrival_copy(0, 0, 0, 1)),
        (k > 1, arrival_copy(0, 0, 1, tm_count + k)),
        (k > 0, arrival_copy(1, 1, 0, tm_count + k)),
    ]
    relay_copies = [
        remote(slot(tm_count + i), slot(i), relay_s.at[i], x_r.at[i], {"tm": 0})
        for i in range(2, tm_count)
    ]
    ext_copy = remote(
        kflat.at[:, pl.ds((block_len - piece) * params, piece * params)], kext, ext_s, ext_r, down
    )
    sends_ext, takes_ext = k > 1, forwards

    loads[0].wait()

    @pl.when(sends_up)
    def _():
        for copy in history_copies:
            copy.start()

    pl.when(k > 0)(lambda: pl.semaphore_wait(ready, 1))
    pl.when(sends_up)(lambda: signal(ready, up))

    for condition, copy in arrival_copies:
        pl.when(condition)(copy.start)

    for copy in loads[1:]:
        copy.wait()
    pl.when(sends_ext)(ext_copy.start)

    @pl.when(k == 0)
    def _():
        for copy in first_pieces:
            copy.wait()

    pl.when(k == 1)(own_piece.wait)

    def receive(c):
        copy = remote(slot(c), slot(c), hist_s.at[0], x_r.at[c], up)
        if c % tm_count == 0 and c < tm_count:
            pl.when(k != 0)(copy.wait_recv)
        elif c == tm_count:
            pl.when(k != 0)(copy.wait_recv)
        elif c == tm_count + 1:
            pl.when(k != 1)(copy.wait_recv)
        elif c == last:
            pl.when(k == 0)(copy.wait_recv)
        else:
            copy.wait_recv() if c < tm_count else pl.when(k != 1)(copy.wait_recv)

    def relay():
        @pl.when(relays)
        def _():
            for i in range(2, tm_count):
                c = tm_count + i
                remote(slot(c), slot(c), hist_s.at[0], x_r.at[c], up).wait_recv()
                relay_copies[i - 2].start()

    def span(c):
        return pl.ds(c * piece, piece)

    def core_copy(c):
        return remote(
            buf0.at[1 - core, :, span(c)], rcv0.at[:, span(c)], s0.at[c], r0.at[c],
            {"par": partner},
        )

    def chip_copy(c, d):
        target = flipped(d)
        return remote(
            mid.at[target, span(c)], mrcv.at[d - 1, span(c)], ms.at[c, d - 1], mr.at[c, d - 1],
            {"par": target * 2 + core},
        )

    def tm_copy(c, d):
        target = lax.rem(k + d, tm_count)
        place = pl.ds(c * piece * rows, piece * rows)
        return remote(
            zbuf.at[target, place], zrcv.at[d - 1, place], zs.at[c, d - 1], zr.at[c, d - 1],
            {"tm": target},
        )

    def compute(c):
        receive(c)
        if c < tm_count - 1:
            pl.when(forwards)(forward_copies[c].start)
        if c == last:
            zext[pl.ds(piece - 1, piece)] = xbuf[pl.ds(2 * block_len - piece, piece)]
            pl.when(takes_ext)(
                remote(kext, kext, ext_s, ext_r, down).wait_recv
            )
        for q in range(piece // 2):
            first = c * piece + 2 * q + 1
            left = xbuf[pl.ds(first, block_len)].reshape(block_len * params, fields)
            right = xbuf[pl.ds(first + 1, block_len)].reshape(block_len * params, fields)
            both = jnp.concatenate([left, right], 1)
            total = jnp.dot(kflat[...], both, preferred_element_type=F32)
            if c == last:
                left = zext[pl.ds(2 * q, piece)].reshape(piece * params, fields)
                right = zext[pl.ds(2 * q + 1, piece)].reshape(piece * params, fields)
                both = jnp.concatenate([left, right], 1)
                total = total + jnp.dot(kext[...], both, preferred_element_type=F32)
            for side in range(2):
                mine = total[:, side * fields : (side + 1) * fields]
                moved = jnp.concatenate([mine[o * rows : (o + 1) * rows] for o in order], 0)
                moved = moved.astype(BF16)
                for n in range(2 * group):
                    part = moved[n * share : (n + 1) * share]
                    buf0[n // group, n % group, c * piece + 2 * q + side] = part
        core_copy(c).start()

    def across(c):
        core_copy(c).wait_recv()
        total = buf0[core, :, span(c)].astype(F32) + rcv0[:, span(c)].astype(F32)
        mid[:, span(c)] = total.astype(BF16)
        for d in flips:
            chip_copy(c, d).start()

    def goes_up(d):
        return k + d < tm_count

    def spread(c):
        total = mid[chip, span(c)].astype(F32)
        for d in range(1, group):
            chip_copy(c, d).wait_recv()
            total = total + mrcv[d - 1, span(c)].astype(F32)
        for t in range(tm_count):
            parts = [total[g, t * rows : (t + 1) * rows] for g in range(piece)]
            zbuf[t, pl.ds(c * piece * rows, piece * rows)] = jnp.concatenate(parts, 0).astype(BF16)
        for d in range(1, tm_count):
            pl.when(jnp.logical_not(goes_up(d)))(tm_copy(c, d).start)

    def rise(c):
        for d in range(1, tm_count):
            pl.when(goes_up(d))(tm_copy(c, d).start)

    def finish(c):
        place = pl.ds(c * piece * rows, piece * rows)
        total = zbuf[k, place].astype(F32)
        for d in range(1, tm_count):
            tm_copy(c, d).wait_recv()
            total = total + zrcv[d - 1, place].astype(F32)
        begin = (c % tm_count) * piece
        out_ref[c // tm_count, begin : begin + piece] = total.reshape(piece, rows, fields).astype(
            out_ref.dtype
        )

    plan = []
    for c in range(last):
        plan += [(compute, c), (across, c)]
        if c == 1:
            plan.append((relay, None))
        if c >= 2:
            plan.append((spread, c - 2))
    plan.insert(-2, (compute, last))
    plan += [(rise, c) for c in range(last - 2)]
    for c in range(last - 2, last):
        plan += [(spread, c), (rise, c)]
    plan.insert(-2, (across, last))
    plan += [(spread, last), (rise, last)]
    plan += [(finish, c) for c in range(pieces)]
    for stage, c in plan:
        if c is None:
            stage()
        else:
            stage(c)

    @pl.when(sends_up)
    def _():
        for copy in history_copies:
            copy.wait_send()

    @pl.when(forwards)
    def _():
        for copy in forward_copies:
            copy.wait_send()

    for condition, copy in arrival_copies:
        pl.when(condition)(copy.wait_send)

    @pl.when(relays)
    def _():
        for copy in relay_copies:
            copy.wait_send()

    pl.when(sends_ext)(ext_copy.wait_send)
    for c in range(pieces):
        core_copy(c).wait_send()
        for d in range(1, group):
            chip_copy(c, d).wait_send()
        for d in range(1, tm_count):
            tm_copy(c, d).wait_send()


def fused(tm_count, group, kernel, history, arrivals):
    block_len, sensors, params = kernel.shape
    fields = history.shape[2]
    steps = arrivals.shape[0]
    piece = block_len // tm_count
    pieces = steps * tm_count
    outputs = steps * block_len
    share = sensors // (2 * group)
    rows = share // tm_count
    dma = pltpu.SemaphoreType.DMA
    scratch = [
        pltpu.VMEM((sensors, block_len * params), BF16),
        pltpu.VMEM((sensors, piece * params), BF16),
        pltpu.VMEM(((steps + 1) * block_len, params, fields), BF16),
        pltpu.VMEM((2 * piece - 1, params, fields), BF16),
        pltpu.VMEM((2, group, outputs, share, fields), BF16),
        pltpu.VMEM((group, outputs, share, fields), BF16),
        pltpu.VMEM((group, outputs, share, fields), BF16),
        pltpu.VMEM((group - 1, outputs, share, fields), BF16),
        pltpu.VMEM((tm_count, outputs * rows, fields), BF16),
        pltpu.VMEM((tm_count - 1, outputs * rows, fields), BF16),
        dma((block_len + 1 + steps,)),
        dma((tm_count,)),
        dma((tm_count,)),
        dma((2,)),
        dma((tm_count,)),
        dma(()),
        dma((pieces,)),
        dma(()),
        dma((pieces,)),
        dma((pieces,)),
        dma((pieces, group - 1)),
        dma((pieces, group - 1)),
        dma((pieces, tm_count - 1)),
        dma((pieces, tm_count - 1)),
        pltpu.SemaphoreType.REGULAR,
    ]
    out_bytes = steps * block_len * rows * fields * 2
    return pl.pallas_call(
        functools.partial(kernel_body, tm_count, group),
        out_shape=pltpu.VMEM((steps, block_len, rows, fields), BF16),
        in_specs=[pl.BlockSpec(memory_space=pltpu.HBM)] * 3,
        out_specs=pl.BlockSpec(memory_space=pltpu.VMEM),
        scratch_shapes=scratch,
        compiler_params=pltpu.CompilerParams(
            collective_id=0, has_side_effects=True, vmem_limit_bytes=VMEM_BYTES - 2 * out_bytes
        ),
    )(kernel, history, arrivals)


def plain(tm_count, kernel, history, arrivals):
    block_len, sensors, params = kernel.shape
    fields = history.shape[2]
    steps = arrivals.shape[0]
    incoming = lax.all_gather(arrivals, "tm", axis=1, tiled=True)
    position = lax.axis_index("tm")
    pairs = [(i, i + 1) for i in range(tm_count - 1)]
    blocks = [history]
    for s in range(steps):
        shifted = lax.ppermute(blocks[-1], "tm", pairs)
        blocks.append(jnp.where(position == 0, incoming[s], shifted))
    window = jnp.concatenate(blocks, 0)
    flat = kernel[::-1].transpose(1, 0, 2).reshape(sensors, block_len * params)

    def one(first):
        part = lax.dynamic_slice_in_dim(window, first, block_len, 0)
        part = part.reshape(block_len * params, fields)
        return jnp.dot(flat, part, preferred_element_type=F32)

    partial = lax.map(one, jnp.arange(steps * block_len, dtype=jnp.int32) + 1)
    partial = partial.reshape(steps, block_len, sensors, fields)
    total = lax.psum_scatter(partial, ("tm", "par"), scatter_dimension=2, tiled=True)
    return total.astype(BF16)


def solution(mesh):
    tm_count, par_count = mesh.shape["tm"], mesh.shape["par"]

    def per_device(kernel, history, arrivals):
        rows = kernel.shape[1] // (tm_count * par_count)
        piece = kernel.shape[0] // tm_count
        fits = rows % 8 == 0 and piece % 2 == 0 and tm_count > 2 and arrivals.shape[0] == 2
        if fits and par_count > 2 and par_count.bit_count() == 1:
            return fused(tm_count, par_count // 2, kernel, history, arrivals)
        return plain(tm_count, kernel, history, arrivals)

    in_specs = (P("tm", None, "par"), P("tm", "par", None), P(None, "tm", "par", None))
    out_specs = P(None, None, ("tm", "par"), None)
    return jax.shard_map(
        per_device, mesh=mesh, in_specs=in_specs, out_specs=out_specs, check_vma=False
    )
```

```python
import functools

import jax
import jax.numpy as jnp
from jax import lax
from jax.experimental import pallas as pl
from jax.experimental.pallas import tpu as pltpu
from jax.sharding import PartitionSpec as P

MESH = pl.DeviceIdType.MESH
F32 = jnp.float32
BF16 = jnp.bfloat16
VMEM_BYTES = 67_043_328


def kernel_body(
    tm_count, group, k_ref, h_ref, a_ref, out_ref, kflat, kext, xbuf, zext, buf0, rcv0, mid, mrcv,
    zbuf, zrcv, load_s, hist_s, fwd_s, arr_s, relay_s, ext_s, x_r, ext_r, s0, r0, ms, mr, zs, zr,
    ready, near
):
    block_len, sensors, params = k_ref.shape
    fields = xbuf.shape[2]
    steps = out_ref.shape[0]
    piece = block_len // tm_count
    pieces = steps * tm_count
    last = pieces - 1
    rows = sensors // (tm_count * group * 2)
    share = sensors // (2 * group)
    k = lax.axis_index("tm")
    par = lax.axis_index("par")
    core, chip = par % 2, par // 2
    partner = par + 1 - 2 * core
    flips = sorted(range(1, group), key=lambda flip: -flip.bit_count())
    top = tm_count - 1

    def flipped(flip):
        target = chip
        for b in range(flip.bit_length()):
            if flip >> b & 1:
                target = target + (1 - 2 * ((chip // (1 << b)) % 2)) * (1 << b)
        return target

    order = [
        (tm * group + q) * 2 + half
        for half in range(2)
        for q in range(group)
        for tm in range(tm_count)
    ]

    def remote(src, dst, send, recv, where):
        return pltpu.make_async_remote_copy(
            src_ref=src, dst_ref=dst, send_sem=send, recv_sem=recv, device_id=where,
            device_id_type=MESH,
        )

    def signal(sem, where):
        pl.semaphore_signal(sem, inc=1, device_id=where, device_id_type=MESH)

    barrier = pltpu.get_barrier_semaphore()
    bits = [1 << b for b in range(group.bit_length() - 1)]
    pl.when(k > 0)(lambda: signal(barrier, {"tm": jnp.maximum(k - 1, 0)}))
    for d in bits:
        signal(barrier, {"par": flipped(d) * 2 + core})
    signal(barrier, {"par": partner})

    history_load = pltpu.make_async_copy(h_ref, xbuf.at[pl.ds(0, block_len)], load_s.at[0])
    kernel_loads = [
        pltpu.make_async_copy(
            k_ref.at[block_len - 1 - j], kflat.at[:, pl.ds(j * params, params)], load_s.at[1]
        )
        for j in range(block_len)
    ]
    first_pieces = []
    for s in range(steps):
        place = xbuf.at[pl.ds(block_len * (s + 1), piece)]
        first_pieces.append(pltpu.make_async_copy(a_ref.at[s], place, load_s.at[2 + s]))
    place = xbuf.at[pl.ds(2 * block_len + piece, piece)]
    own_piece = pltpu.make_async_copy(a_ref.at[0], place, load_s.at[2])

    history_load.start()
    for copy in kernel_loads:
        copy.start()

    @pl.when(k == 0)
    def _():
        for copy in first_pieces:
            copy.start()

    pl.when(k == 1)(own_piece.start)

    @pl.when((k == 0) | (k == top))
    def _():
        kext[...] = jnp.zeros_like(kext)

    @pl.when(k > 1)
    def _():
        tail = xbuf.at[pl.ds(block_len + last * piece, piece)]
        tail[...] = jnp.zeros(tail.shape, BF16)

    zext[pl.ds(0, piece - 1)] = jnp.zeros((piece - 1, params, fields), BF16)

    pl.semaphore_wait(barrier, 1 + len(bits) + (k < top).astype(jnp.int32))

    def slot(c):
        return xbuf.at[pl.ds(block_len + c * piece, piece)]

    up, down = {"tm": jnp.minimum(k + 1, top)}, {"tm": jnp.maximum(k - 1, 0)}
    sends_up = k < top
    forwards = (k > 0) & (k < top)

    history_copies = [
        remote(xbuf.at[pl.ds(i * piece, piece)], slot(i), hist_s, x_r.at[i], up)
        for i in range(tm_count)
    ]
    forward_copies = [
        remote(slot(i), slot(i + tm_count), fwd_s, x_r.at[i + tm_count], up)
        for i in range(tm_count - 1)
    ]

    def arrival_copy(n, s, target, c):
        return remote(a_ref.at[s], slot(c), arr_s.at[n], x_r.at[c], {"tm": target})

    arrival_copies = [
        (k % 2 == 0, arrival_copy(0, 0, 1, tm_count + k)),
        (k % 2 == 1, arrival_copy(0, 0, 0, k)),
        (k > 0, arrival_copy(1, 1, 0, tm_count + k)),
    ]
    evens, odds = range(2, tm_count, 2), range(3, tm_count, 2)
    relay_copies = {
        i: remote(slot(tm_count + i), slot(i), relay_s, x_r.at[i], {"tm": 0}) for i in evens
    } | {
        i: remote(slot(i), slot(tm_count + i), relay_s, x_r.at[tm_count + i], {"tm": 1})
        for i in odds
    }
    ext_copy = remote(
        kflat.at[:, pl.ds((block_len - piece) * params, piece * params)], kext, ext_s, ext_r, down
    )
    sends_ext, takes_ext = k > 1, forwards

    history_load.wait()

    @pl.when(sends_up)
    def _():
        for copy in history_copies:
            copy.start()

    pl.when(k > 0)(lambda: pl.semaphore_wait(ready, 1))
    pl.when(sends_up)(lambda: signal(ready, up))

    for condition, copy in arrival_copies:
        pl.when(condition)(copy.start)

    if bits[1:]:
        signal(near.at[0], {"par": flipped(1) * 2 + core})

    pltpu.make_async_copy(kflat, kflat, load_s.at[1]).wait()
    pl.when(sends_ext)(ext_copy.start)

    @pl.when(k == 0)
    def _():
        for copy in first_pieces:
            copy.wait()

    pl.when(k == 1)(own_piece.wait)

    for n, d in enumerate(bits[:-1]):
        pl.semaphore_wait(near.at[n], 1)
        if n + 1 < len(bits) - 1:
            signal(near.at[n + 1], {"par": flipped(bits[n + 1]) * 2 + core})

    def taken(c):
        return remote(slot(c), slot(c), hist_s, x_r.at[c], up)

    def receive(c):
        i = c % tm_count
        waits = k >= 0
        if i == c:
            waits = (k != 0) if c == 0 else waits
        elif i < 2:
            waits = k != i
        elif i % 2 == 0:
            waits = k != 1
        if c == last:
            waits = waits & (k < 2)
        pl.when(waits)(taken(c).wait_recv)
        if c in odds:
            pl.when(k == 0)(relay_copies[c].start)

    def relay():
        @pl.when(k == 1)
        def _():
            for i in evens:
                taken(tm_count + i).wait_recv()
                relay_copies[i].start()

    def span(c):
        return pl.ds(c * piece, piece)

    def core_copy(c):
        return remote(
            buf0.at[1 - core, :, span(c)], rcv0.at[:, span(c)], s0, r0.at[c],
            {"par": partner},
        )

    def chip_copy(c, d):
        target = flipped(d)
        return remote(
            mid.at[target, span(c)], mrcv.at[d - 1, span(c)], ms, mr.at[c],
            {"par": target * 2 + core},
        )

    def tm_copy(c, d):
        target = lax.rem(k + d, tm_count)
        place = pl.ds(c * piece * rows, piece * rows)
        return remote(
            zbuf.at[target, place], zrcv.at[d - 1, place], zs, zr.at[c],
            {"tm": target},
        )

    def compute(c):
        receive(c)
        if c < tm_count - 1:
            pl.when(forwards)(forward_copies[c].start)
        if c == last:
            zext[pl.ds(piece - 1, piece)] = xbuf[pl.ds(2 * block_len - piece, piece)]
            pl.when(takes_ext)(
                remote(kext, kext, ext_s, ext_r, down).wait_recv
            )
        for q in range(piece // 2):
            first = c * piece + 2 * q + 1
            left = xbuf[pl.ds(first, block_len)].reshape(block_len * params, fields)
            right = xbuf[pl.ds(first + 1, block_len)].reshape(block_len * params, fields)
            both = jnp.concatenate([left, right], 1)
            total = jnp.dot(kflat[...], both, preferred_element_type=F32)
            if c == last:
                left = zext[pl.ds(2 * q, piece)].reshape(piece * params, fields)
                right = zext[pl.ds(2 * q + 1, piece)].reshape(piece * params, fields)
                both = jnp.concatenate([left, right], 1)
                total = total + jnp.dot(kext[...], both, preferred_element_type=F32)
            for side in range(2):
                mine = total[:, side * fields : (side + 1) * fields]
                moved = jnp.concatenate([mine[o * rows : (o + 1) * rows] for o in order], 0)
                moved = moved.astype(BF16)
                for n in range(2 * group):
                    part = moved[n * share : (n + 1) * share]
                    buf0[n // group, n % group, c * piece + 2 * q + side] = part
        core_copy(c).start()

    def across(c):
        core_copy(c).wait_recv()
        total = buf0[core, :, span(c)].astype(F32) + rcv0[:, span(c)].astype(F32)
        mid[:, span(c)] = total.astype(BF16)
        for d in flips:
            chip_copy(c, d).start()

    def goes_up(d):
        return k + d < tm_count

    def spread(c):
        total = mid[chip, span(c)].astype(F32)
        place = mrcv.at[:, span(c)]
        remote(place, place, ms, mr.at[c], {"par": par}).wait_recv()
        for d in range(1, group):
            total = total + mrcv[d - 1, span(c)].astype(F32)
        for t in range(tm_count):
            parts = [total[g, t * rows : (t + 1) * rows] for g in range(piece)]
            zbuf[t, pl.ds(c * piece * rows, piece * rows)] = jnp.concatenate(parts, 0).astype(BF16)
        for d in range(1, tm_count):
            pl.when(jnp.logical_not(goes_up(d)))(tm_copy(c, d).start)

    def rise(c):
        for d in range(1, tm_count):
            pl.when(goes_up(d))(tm_copy(c, d).start)

    def finish(c):
        place = pl.ds(c * piece * rows, piece * rows)
        total = zbuf[k, place].astype(F32)
        taken_parts = zrcv.at[:, place]
        remote(taken_parts, taken_parts, zs, zr.at[c], {"tm": k}).wait_recv()
        for d in range(1, tm_count):
            total = total + zrcv[d - 1, place].astype(F32)
        begin = (c % tm_count) * piece
        out_ref[c // tm_count, begin : begin + piece] = total.reshape(piece, rows, fields).astype(
            out_ref.dtype
        )

    plan = []
    for c in range(last):
        plan += [(compute, c), (across, c)]
        if c == 1:
            plan.append((relay, None))
        if c >= 2:
            plan.append((spread, c - 2))
    plan.insert(-2, (compute, last))
    plan += [(rise, c) for c in range(last - 2)]
    for c in range(last - 2, last):
        plan += [(spread, c), (rise, c)]
    plan.insert(-2, (across, last))
    plan += [(spread, last), (rise, last)]
    plan += [(finish, c) for c in range(pieces)]
    for stage, c in plan:
        if c is None:
            stage()
        else:
            stage(c)

    def sent(place, sem):
        return remote(place, place, sem, x_r.at[0], up).wait_send

    pl.when(sends_up)(sent(xbuf.at[pl.ds(0, block_len)], hist_s))
    pl.when(forwards)(sent(xbuf.at[pl.ds(0, block_len - piece)], fwd_s))
    for condition, copy in arrival_copies:
        pl.when(condition)(copy.wait_send)
    for step, those in ((1, evens), (0, odds)):
        if those:
            pl.when(k == step)(sent(xbuf.at[pl.ds(0, len(those) * piece)], relay_s))
    pl.when(sends_ext)(ext_copy.wait_send)
    sent(rcv0, s0)()
    sent(mrcv, ms)()
    sent(zrcv, zs)()


def fused(tm_count, group, kernel, history, arrivals):
    block_len, sensors, params = kernel.shape
    fields = history.shape[2]
    steps = arrivals.shape[0]
    piece = block_len // tm_count
    pieces = steps * tm_count
    outputs = steps * block_len
    share = sensors // (2 * group)
    rows = share // tm_count
    dma = pltpu.SemaphoreType.DMA
    scratch = [
        pltpu.VMEM((sensors, block_len * params), BF16),
        pltpu.VMEM((sensors, piece * params), BF16),
        pltpu.VMEM(((steps + 1) * block_len, params, fields), BF16),
        pltpu.VMEM((2 * piece - 1, params, fields), BF16),
        pltpu.VMEM((2, group, outputs, share, fields), BF16),
        pltpu.VMEM((group, outputs, share, fields), BF16),
        pltpu.VMEM((group, outputs, share, fields), BF16),
        pltpu.VMEM((group - 1, outputs, share, fields), BF16),
        pltpu.VMEM((tm_count, outputs * rows, fields), BF16),
        pltpu.VMEM((tm_count - 1, outputs * rows, fields), BF16),
        dma((2 + steps,)),
        dma(()),
        dma(()),
        dma((2,)),
        dma(()),
        dma(()),
        dma((pieces,)),
        dma(()),
        dma(()),
        dma((pieces,)),
        dma(()),
        dma((pieces,)),
        dma(()),
        dma((pieces,)),
        pltpu.SemaphoreType.REGULAR,
        pltpu.SemaphoreType.REGULAR((max(group.bit_length() - 2, 1),)),
    ]
    out_bytes = steps * block_len * rows * fields * 2
    return pl.pallas_call(
        functools.partial(kernel_body, tm_count, group),
        out_shape=pltpu.VMEM((steps, block_len, rows, fields), BF16),
        in_specs=[pl.BlockSpec(memory_space=pltpu.HBM)] * 3,
        out_specs=pl.BlockSpec(memory_space=pltpu.VMEM),
        scratch_shapes=scratch,
        compiler_params=pltpu.CompilerParams(
            collective_id=0, has_side_effects=True, vmem_limit_bytes=VMEM_BYTES - 2 * out_bytes
        ),
    )(kernel, history, arrivals)


def plain(tm_count, kernel, history, arrivals):
    block_len, sensors, params = kernel.shape
    fields = history.shape[2]
    steps = arrivals.shape[0]
    incoming = lax.all_gather(arrivals, "tm", axis=1, tiled=True)
    position = lax.axis_index("tm")
    pairs = [(i, i + 1) for i in range(tm_count - 1)]
    blocks = [history]
    for s in range(steps):
        shifted = lax.ppermute(blocks[-1], "tm", pairs)
        blocks.append(jnp.where(position == 0, incoming[s], shifted))
    window = jnp.concatenate(blocks, 0)
    flat = kernel[::-1].transpose(1, 0, 2).reshape(sensors, block_len * params)

    def one(first):
        part = lax.dynamic_slice_in_dim(window, first, block_len, 0)
        part = part.reshape(block_len * params, fields)
        return jnp.dot(flat, part, preferred_element_type=F32)

    partial = lax.map(one, jnp.arange(steps * block_len, dtype=jnp.int32) + 1)
    partial = partial.reshape(steps, block_len, sensors, fields)
    total = lax.psum_scatter(partial, ("tm", "par"), scatter_dimension=2, tiled=True)
    return total.astype(BF16)


def solution(mesh):
    tm_count, par_count = mesh.shape["tm"], mesh.shape["par"]

    def per_device(kernel, history, arrivals):
        rows = kernel.shape[1] // (tm_count * par_count)
        piece = kernel.shape[0] // tm_count
        fits = rows % 8 == 0 and piece % 2 == 0 and tm_count > 2 and arrivals.shape[0] == 2
        if fits and par_count > 2 and par_count.bit_count() == 1:
            return fused(tm_count, par_count // 2, kernel, history, arrivals)
        return plain(tm_count, kernel, history, arrivals)

    in_specs = (P("tm", None, "par"), P("tm", "par", None), P(None, "tm", "par", None))
    out_specs = P(None, None, ("tm", "par"), None)
    return jax.shard_map(
        per_device, mesh=mesh, in_specs=in_specs, out_specs=out_specs, check_vma=False
    )
```

```python
import functools

import jax
import jax.numpy as jnp
from jax import lax
from jax.experimental import pallas as pl
from jax.experimental.pallas import tpu as pltpu
from jax.sharding import PartitionSpec as P

MESH = pl.DeviceIdType.MESH
F32 = jnp.float32
BF16 = jnp.bfloat16
VMEM_BYTES = 67_043_328
LATE = 2


def kernel_body(
    tm_count, group, k_ref, h_ref, a_ref, out_ref, kflat, kext, xbuf, abuf, zext, acc, buf0, rcv0, mid, mrcv,
    zbuf, zrcv, load_s, hist_s, fwd_s, arr_s, relay_s, ext_s, x_r, ext_r, s0, r0, ms, mr, zs, zr,
    ready, near
):
    block_len, sensors, params = k_ref.shape
    fields = xbuf.shape[2]
    steps = out_ref.shape[0]
    piece = block_len // tm_count
    pieces = steps * tm_count
    last = pieces - 1
    half = piece // 2
    split = last - 1
    spans = [(c * piece, piece) for c in range(split)]
    spans += [(split * piece, half), (split * piece + half, piece - half), (last * piece, piece)]
    chunks = len(spans)
    rows = sensors // (tm_count * group * 2)
    share = sensors // (2 * group)
    k = lax.axis_index("tm")
    par = lax.axis_index("par")
    core, chip = par % 2, par // 2
    partner = par + 1 - 2 * core
    flips = sorted(range(1, group), key=lambda flip: -flip.bit_count())
    top = tm_count - 1

    def flipped(flip):
        target = chip
        for b in range(flip.bit_length()):
            if flip >> b & 1:
                target = target + (1 - 2 * ((chip // (1 << b)) % 2)) * (1 << b)
        return target

    order = [
        (tm * group + q) * 2 + half
        for half in range(2)
        for q in range(group)
        for tm in range(tm_count)
    ]

    def remote(src, dst, send, recv, where):
        return pltpu.make_async_remote_copy(
            src_ref=src, dst_ref=dst, send_sem=send, recv_sem=recv, device_id=where,
            device_id_type=MESH,
        )

    def signal(sem, where):
        pl.semaphore_signal(sem, inc=1, device_id=where, device_id_type=MESH)

    barrier = pltpu.get_barrier_semaphore()
    bits = [1 << b for b in range(group.bit_length() - 1)]
    pl.when(k > 0)(lambda: signal(barrier, {"tm": jnp.maximum(k - 1, 0)}))
    pl.when(k < top)(lambda: signal(barrier, {"tm": jnp.minimum(k + 1, top)}))
    for d in bits:
        signal(barrier, {"par": flipped(d) * 2 + core})
    signal(barrier, {"par": partner})

    history_load = pltpu.make_async_copy(h_ref, xbuf.at[pl.ds(0, block_len)], load_s.at[0])
    kernel_loads = [
        pltpu.make_async_copy(
            k_ref.at[block_len - 1 - j], kflat.at[:, pl.ds(j * params, params)], load_s.at[1]
        )
        for j in range(block_len)
    ]
    first_pieces = []
    for s in range(steps):
        place = xbuf.at[pl.ds(block_len * (s + 1), piece)]
        first_pieces.append(pltpu.make_async_copy(a_ref.at[s], place, load_s.at[2 + s]))
    place = xbuf.at[pl.ds(2 * block_len + piece, piece)]
    own_piece = pltpu.make_async_copy(a_ref.at[0], place, load_s.at[2])

    arrival_load = pltpu.make_async_copy(a_ref, abuf, load_s.at[2 + steps])

    history_load.start()
    arrival_load.start()
    for copy in kernel_loads:
        copy.start()

    @pl.when(k == 0)
    def _():
        for copy in first_pieces:
            copy.start()

    pl.when(k == 1)(own_piece.start)

    @pl.when((k == 0) | (k == top))
    def _():
        kext[...] = jnp.zeros_like(kext)

    @pl.when(k > 1)
    def _():
        tail = xbuf.at[pl.ds(block_len + last * piece, piece)]
        tail[...] = jnp.zeros(tail.shape, BF16)

    zext[pl.ds(0, piece - 1)] = jnp.zeros((piece - 1, params, fields), BF16)

    around = (k < top).astype(jnp.int32) + (k > 0).astype(jnp.int32)
    pl.semaphore_wait(barrier, 1 + len(bits) + around)

    def slot(c):
        return xbuf.at[pl.ds(block_len + c * piece, piece)]

    up, down = {"tm": jnp.minimum(k + 1, top)}, {"tm": jnp.maximum(k - 1, 0)}
    sends_up = k < top
    forwards = (k > 0) & (k < top)

    history_copies = [
        remote(xbuf.at[pl.ds(i * piece, piece)], slot(i), hist_s, x_r.at[i], up)
        for i in range(tm_count)
    ]

    def parts(c):
        if c == split:
            return [(0, half, c), (half, piece - half, pieces)]
        return [(0, piece, c)]

    def into(c, src, send, where):
        return [
            remote(
                src.at[pl.ds(first, count)],
                xbuf.at[pl.ds(block_len + c * piece + first, count)],
                send, x_r.at[sem], where,
            )
            for first, count, sem in parts(c)
        ]

    forward_copies = [
        into(i + tm_count, slot(i), fwd_s, up) for i in range(tm_count - 1)
    ]

    def arrivals_from(step, s, target, c):
        copies = into(c, abuf.at[s], arr_s.at[s], {"tm": target})
        return [(k == step, copy) for copy in copies]

    near_copies = arrivals_from(0, 0, 1, tm_count)
    near_copies += arrivals_from(1, 0, 0, 1) + arrivals_from(1, 1, 0, tm_count + 1)
    near_copies += arrivals_from(2, 0, 1, tm_count + 2)
    far_copies, late_copies = [], []
    for i in range(2, tm_count):
        if i > 2:
            far_copies += arrivals_from(i, 0, (i + 1) % 2, i if i % 2 else tm_count + i)
        late_copies += arrivals_from(i, 1, 0, tm_count + i)
    evens, odds = range(2, tm_count, 2), range(3, tm_count, 2)
    relay_copies = {
        i: remote(slot(tm_count + i), slot(i), relay_s, x_r.at[i], {"tm": 0}) for i in evens
    } | {
        i: remote(slot(i), slot(tm_count + i), relay_s, x_r.at[tm_count + i], {"tm": 1})
        for i in odds
    }
    ext_copy = remote(
        kflat.at[:, pl.ds((block_len - piece) * params, piece * params)], kext, ext_s, ext_r, down
    )
    sends_ext, takes_ext = k > 1, forwards

    history_load.wait()

    @pl.when(sends_up)
    def _():
        for copy in history_copies:
            copy.start()

    arrival_load.wait()
    for condition, copy in near_copies:
        pl.when(condition)(copy.start)

    pl.when(k > 0)(lambda: pl.semaphore_wait(ready, 1))
    pl.when(sends_up)(lambda: signal(ready, up))

    for condition, copy in far_copies:
        pl.when(condition)(copy.start)

    if bits[1:]:
        signal(near.at[0], {"par": flipped(1) * 2 + core})

    pltpu.make_async_copy(kflat, kflat, load_s.at[1]).wait()
    pl.when(sends_ext)(ext_copy.start)

    @pl.when(k == 0)
    def _():
        for copy in first_pieces:
            copy.wait()

    pl.when(k == 1)(own_piece.wait)

    for n, d in enumerate(bits[:-1]):
        pl.semaphore_wait(near.at[n], 1)
        if n + 1 < len(bits) - 1:
            signal(near.at[n + 1], {"par": flipped(bits[n + 1]) * 2 + core})

    def taken(unit):
        c = split if unit == pieces else unit
        first, count = [(f, n) for f, n, sem in parts(c) if sem == unit][0]
        place = xbuf.at[pl.ds(block_len + c * piece + first, count)]
        return remote(place, place, hist_s, x_r.at[unit], up)

    def receive(unit):
        c = split if unit == pieces else unit
        i = c % tm_count
        waits = k >= 0
        if i == c:
            waits = (k != 0) if c == 0 or c in odds else waits
        elif i < 2:
            waits = k != i
        elif i % 2 == 0:
            waits = k != 1
        if c == last:
            waits = waits & (k < 2)
        pl.when(waits)(taken(unit).wait_recv)

    def relay():
        @pl.when(k == 1)
        def _():
            for i in evens:
                for _, _, unit in parts(tm_count + i):
                    taken(unit).wait_recv()
                relay_copies[i].start()

        @pl.when(k == 0)
        def _():
            for i in odds:
                taken(i).wait_recv()
                relay_copies[i].start()

    def late():
        for condition, copy in late_copies:
            pl.when(condition)(copy.start)

    def span(c):
        return pl.ds(*spans[c])

    def flat_span(c):
        first, count = spans[c]
        return pl.ds(first * rows, count * rows)

    def core_copy(c):
        return remote(
            buf0.at[1 - core, :, span(c)], rcv0.at[:, span(c)], s0, r0.at[c],
            {"par": partner},
        )

    def chip_copy(c, d):
        target = flipped(d)
        return remote(
            mid.at[target, span(c)], mrcv.at[d - 1, span(c)], ms, mr.at[c],
            {"par": target * 2 + core},
        )

    def tm_copy(c, d):
        target = lax.rem(k + d, tm_count)
        place = flat_span(c)
        return remote(
            zbuf.at[target, place], zrcv.at[d - 1, place], zs, zr.at[c],
            {"tm": target},
        )

    def product(r, low, high):
        count = (high - low) * params
        left = xbuf[pl.ds(r + 1 + low, high - low)].reshape(count, fields)
        right = xbuf[pl.ds(r + 2 + low, high - low)].reshape(count, fields)
        both = jnp.concatenate([left, right], 1)
        lags = kflat[:, low * params : high * params]
        return jnp.dot(lags, both, preferred_element_type=F32)

    def hand_over(r, total):
        for side in range(2):
            mine = total[:, side * fields : (side + 1) * fields]
            moved = jnp.concatenate([mine[o * rows : (o + 1) * rows] for o in order], 0)
            moved = moved.astype(BF16)
            for n in range(2 * group):
                buf0[n // group, n % group, r + side] = moved[n * share : (n + 1) * share]

    def compute(c):
        receive(c)
        if c < tm_count - 1:

            @pl.when(forwards)
            def _():
                for copy in forward_copies[c]:
                    copy.start()

        first, count = spans[c]
        for r in range(first, first + count, 2):
            hand_over(r, product(r, 0, block_len))
        core_copy(c).start()

    begin = spans[split + 1][0]
    last_rows = range(begin, steps * block_len, 2)

    def bound(r, c):
        return block_len + c * piece - r - 2

    def early():
        zext[pl.ds(piece - 1, piece)] = xbuf[pl.ds(2 * block_len - piece, piece)]
        pl.when(takes_ext)(remote(kext, kext, ext_s, ext_r, down).wait_recv)
        for n, r in enumerate(last_rows):
            total = product(r, 0, bound(r, split - 1))
            t = r - last * piece
            if t >= 0:
                left = zext[pl.ds(t, piece)].reshape(piece * params, fields)
                right = zext[pl.ds(t + 1, piece)].reshape(piece * params, fields)
                both = jnp.concatenate([left, right], 1)
                total = total + jnp.dot(kext[...], both, preferred_element_type=F32)
            acc[n] = total

    def middle():
        for n, r in enumerate(last_rows):
            acc[n] = acc[n] + product(r, bound(r, split - 1), bound(r, split))

    def final():
        receive(pieces)
        for n, r in enumerate(last_rows):
            if r == last * piece:
                core_copy(split + 1).start()
                receive(last)
            hand_over(r, acc[n] + product(r, bound(r, split), block_len))
        core_copy(split + 2).start()

    def across(c):
        core_copy(c).wait_recv()
        total = buf0[core, :, span(c)].astype(F32) + rcv0[:, span(c)].astype(F32)
        mid[:, span(c)] = total.astype(BF16)
        for d in flips:
            chip_copy(c, d).start()

    def goes_up(d):
        return k + d < tm_count

    def spread(c):
        total = mid[chip, span(c)].astype(F32)
        place = mrcv.at[:, span(c)]
        remote(place, place, ms, mr.at[c], {"par": par}).wait_recv()
        for d in range(1, group):
            total = total + mrcv[d - 1, span(c)].astype(F32)
        for t in range(tm_count):
            mine = [total[g, t * rows : (t + 1) * rows] for g in range(spans[c][1])]
            zbuf[t, flat_span(c)] = jnp.concatenate(mine, 0).astype(BF16)
        for d in range(1, tm_count):
            pl.when(jnp.logical_not(goes_up(d)))(tm_copy(c, d).start)

    def rise(c):
        for d in range(1, tm_count):
            pl.when(goes_up(d))(tm_copy(c, d).start)

    def finish(c):
        place = flat_span(c)
        total = zbuf[k, place].astype(F32)
        taken_parts = zrcv.at[:, place]
        remote(taken_parts, taken_parts, zs, zr.at[c], {"tm": k}).wait_recv()
        for d in range(1, tm_count):
            total = total + zrcv[d - 1, place].astype(F32)
        first, count = spans[c]
        total = total.reshape(count, rows, fields).astype(out_ref.dtype)
        first = first % block_len
        out_ref[spans[c][0] // block_len, first : first + count] = total

    def run(plan):
        for stage, *c in plan:
            stage(*c)

    ends = [(rise, c) for c in range(split - 1)]
    ends += [(across, split + 1), (spread, split - 1), (rise, split - 1), (across, split + 2)]
    for c in range(split, chunks):
        ends += [(spread, c), (rise, c)]

    @pl.when(k == 0)
    def _():
        plan = [(compute, 0), (across, 0), (compute, 1), (relay,), (across, 1), (spread, 0)]
        for c in range(2, split):
            plan.append((compute, c))
            if c > 2:
                plan.append((across, c - 1))
            if c > 3:
                plan.append((spread, c - 3))
        plan += [(early,), (across, split - 1), (spread, split - 3), (middle,), (compute, split)]
        plan += [(spread, split - 2), (final,), (across, split)]
        run(plan + ends)

    @pl.when(k > 0)
    def _():
        plan = []
        for c in range(split):
            plan += [(compute, c), (across, c)]
            if c == 0:
                plan.append((relay,))
            if c == 2:
                plan.append((late,))
            if c >= 2:
                plan.append((spread, c - 2))
            if c == split - 2:
                plan.append((early,))
        plan += [(compute, split), (middle,), (across, split), (spread, split - 2), (final,)]
        run(plan + ends)

    run([(finish, c) for c in range(chunks)])

    def sent(place, sem):
        return remote(place, place, sem, x_r.at[0], up).wait_send

    pl.when(sends_up)(sent(xbuf.at[pl.ds(0, block_len)], hist_s))
    pl.when(forwards)(sent(xbuf.at[pl.ds(0, block_len - piece)], fwd_s))
    sent(abuf.at[0], arr_s.at[0])()
    pl.when(k > 0)(sent(abuf.at[1], arr_s.at[1]))
    for step, those in ((1, evens), (0, odds)):
        if those:
            pl.when(k == step)(sent(xbuf.at[pl.ds(0, len(those) * piece)], relay_s))
    pl.when(sends_ext)(ext_copy.wait_send)
    sent(rcv0, s0)()
    sent(mrcv, ms)()
    sent(zrcv, zs)()


def fused(tm_count, group, kernel, history, arrivals):
    block_len, sensors, params = kernel.shape
    fields = history.shape[2]
    steps = arrivals.shape[0]
    piece = block_len // tm_count
    pieces = steps * tm_count
    outputs = steps * block_len
    share = sensors // (2 * group)
    rows = share // tm_count
    dma = pltpu.SemaphoreType.DMA
    scratch = [
        pltpu.VMEM((sensors, block_len * params), BF16),
        pltpu.VMEM((sensors, piece * params), BF16),
        pltpu.VMEM(((steps + 1) * block_len, params, fields), BF16),
        pltpu.VMEM((steps, piece, params, fields), BF16),
        pltpu.VMEM((2 * piece - 1, params, fields), BF16),
        pltpu.VMEM((piece - piece // 4, sensors, 2 * fields), F32),
        pltpu.VMEM((2, group, outputs, share, fields), BF16),
        pltpu.VMEM((group, outputs, share, fields), BF16),
        pltpu.VMEM((group, outputs, share, fields), BF16),
        pltpu.VMEM((group - 1, outputs, share, fields), BF16),
        pltpu.VMEM((tm_count, outputs * rows, fields), BF16),
        pltpu.VMEM((tm_count - 1, outputs * rows, fields), BF16),
        dma((3 + steps,)),
        dma(()),
        dma(()),
        dma((2,)),
        dma(()),
        dma(()),
        dma((pieces + 1,)),
        dma(()),
        dma(()),
        dma((pieces + 1,)),
        dma(()),
        dma((pieces + 1,)),
        dma(()),
        dma((pieces + 1,)),
        pltpu.SemaphoreType.REGULAR,
        pltpu.SemaphoreType.REGULAR((max(group.bit_length() - 2, 1),)),
    ]
    out_bytes = steps * block_len * rows * fields * 2
    return pl.pallas_call(
        functools.partial(kernel_body, tm_count, group),
        out_shape=pltpu.VMEM((steps, block_len, rows, fields), BF16),
        in_specs=[pl.BlockSpec(memory_space=pltpu.HBM)] * 3,
        out_specs=pl.BlockSpec(memory_space=pltpu.VMEM),
        scratch_shapes=scratch,
        compiler_params=pltpu.CompilerParams(
            collective_id=0, has_side_effects=True, vmem_limit_bytes=VMEM_BYTES - 2 * out_bytes
        ),
    )(kernel, history, arrivals)


def plain(tm_count, kernel, history, arrivals):
    block_len, sensors, params = kernel.shape
    fields = history.shape[2]
    steps = arrivals.shape[0]
    incoming = lax.all_gather(arrivals, "tm", axis=1, tiled=True)
    position = lax.axis_index("tm")
    pairs = [(i, i + 1) for i in range(tm_count - 1)]
    blocks = [history]
    for s in range(steps):
        shifted = lax.ppermute(blocks[-1], "tm", pairs)
        blocks.append(jnp.where(position == 0, incoming[s], shifted))
    window = jnp.concatenate(blocks, 0)
    flat = kernel[::-1].transpose(1, 0, 2).reshape(sensors, block_len * params)

    def one(first):
        part = lax.dynamic_slice_in_dim(window, first, block_len, 0)
        part = part.reshape(block_len * params, fields)
        return jnp.dot(flat, part, preferred_element_type=F32)

    partial = lax.map(one, jnp.arange(steps * block_len, dtype=jnp.int32) + 1)
    partial = partial.reshape(steps, block_len, sensors, fields)
    total = lax.psum_scatter(partial, ("tm", "par"), scatter_dimension=2, tiled=True)
    return total.astype(BF16)


def solution(mesh):
    tm_count, par_count = mesh.shape["tm"], mesh.shape["par"]

    def per_device(kernel, history, arrivals):
        rows = kernel.shape[1] // (tm_count * par_count)
        piece = kernel.shape[0] // tm_count
        fits = rows % 8 == 0 and piece % 4 == 0 and tm_count > 2 and arrivals.shape[0] == 2
        if fits and par_count > 2 and par_count.bit_count() == 1:
            return fused(tm_count, par_count // 2, kernel, history, arrivals)
        return plain(tm_count, kernel, history, arrivals)

    in_specs = (P("tm", None, "par"), P("tm", "par", None), P(None, "tm", "par", None))
    out_specs = P(None, None, ("tm", "par"), None)
    return jax.shard_map(
        per_device, mesh=mesh, in_specs=in_specs, out_specs=out_specs, check_vma=False
    )
```

```python
import functools

import jax
import jax.numpy as jnp
from jax import lax
from jax.experimental import pallas as pl
from jax.experimental.pallas import tpu as pltpu
from jax.sharding import PartitionSpec as P

MESH = pl.DeviceIdType.MESH
F32 = jnp.float32
BF16 = jnp.bfloat16
VMEM_BYTES = 67_043_328
LATE = 2


def kernel_body(
    tm_count, group, k_ref, h_ref, a_ref, out_ref, kflat, kext, xbuf, abuf, zext, acc, buf0, rcv0, mid, mrcv,
    zbuf, zrcv, load_s, hist_s, fwd_s, arr_s, relay_s, ext_s, x_r, ext_r, s0, r0, ms, mr, zs, zr,
    ready, near
):
    block_len, sensors, params = k_ref.shape
    fields = xbuf.shape[2]
    steps = out_ref.shape[0]
    piece = block_len // tm_count
    pieces = steps * tm_count
    last = pieces - 1
    half = piece // 2
    split = last - 1
    spans = [(c * piece, piece) for c in range(split)]
    spans += [(split * piece, half), (split * piece + half, piece - half), (last * piece, piece)]
    chunks = len(spans)
    rows = sensors // (tm_count * group * 2)
    share = sensors // (2 * group)
    k = lax.axis_index("tm")
    par = lax.axis_index("par")
    core, chip = par % 2, par // 2
    partner = par + 1 - 2 * core
    flips = sorted(range(1, group), key=lambda flip: -flip.bit_count())
    top = tm_count - 1

    def flipped(flip):
        target = chip
        for b in range(flip.bit_length()):
            if flip >> b & 1:
                target = target + (1 - 2 * ((chip // (1 << b)) % 2)) * (1 << b)
        return target

    order = [
        (tm * group + q) * 2 + half
        for half in range(2)
        for q in range(group)
        for tm in range(tm_count)
    ]

    def remote(src, dst, send, recv, where):
        return pltpu.make_async_remote_copy(
            src_ref=src, dst_ref=dst, send_sem=send, recv_sem=recv, device_id=where,
            device_id_type=MESH,
        )

    def signal(sem, where):
        pl.semaphore_signal(sem, inc=1, device_id=where, device_id_type=MESH)

    barrier = pltpu.get_barrier_semaphore()
    bits = [1 << b for b in range(group.bit_length() - 1)]
    pl.when(k > 0)(lambda: signal(barrier, {"tm": jnp.maximum(k - 1, 0)}))
    pl.when(k < top)(lambda: signal(barrier, {"tm": jnp.minimum(k + 1, top)}))
    for d in bits:
        signal(barrier, {"par": flipped(d) * 2 + core})
    signal(barrier, {"par": partner})

    history_load = pltpu.make_async_copy(h_ref, xbuf.at[pl.ds(0, block_len)], load_s.at[0])
    kernel_loads = [
        pltpu.make_async_copy(
            k_ref.at[block_len - 1 - j], kflat.at[:, pl.ds(j * params, params)], load_s.at[1]
        )
        for j in range(block_len)
    ]
    first_pieces = []
    for s in range(steps):
        place = xbuf.at[pl.ds(block_len * (s + 1), piece)]
        first_pieces.append(pltpu.make_async_copy(a_ref.at[s], place, load_s.at[2 + s]))
    place = xbuf.at[pl.ds(2 * block_len + piece, piece)]
    own_piece = pltpu.make_async_copy(a_ref.at[0], place, load_s.at[2])

    arrival_load = pltpu.make_async_copy(a_ref, abuf, load_s.at[2 + steps])

    history_load.start()
    arrival_load.start()
    for copy in kernel_loads:
        copy.start()

    @pl.when(k == 0)
    def _():
        for copy in first_pieces:
            copy.start()

    pl.when(k == 1)(own_piece.start)

    wide = 2 * piece
    @pl.when((k > 0) & (k < top - 1))
    def _():
        kext[:, pl.ds(0, piece * params)] = jnp.zeros((sensors, piece * params), BF16)

    @pl.when((k > 1) & (k < top))
    def _():
        tail = xbuf.at[pl.ds(block_len + last * piece, piece)]
        tail[...] = jnp.zeros(tail.shape, BF16)

    @pl.when(k == top)
    def _():
        xbuf[pl.ds(block_len + split * piece, 1)] = jnp.zeros((1, params, fields), BF16)

    zext[pl.ds(0, wide - 1 + piece)] = jnp.zeros((wide - 1 + piece, params, fields), BF16)

    around = (k < top).astype(jnp.int32) + (k > 0).astype(jnp.int32)
    pl.semaphore_wait(barrier, 1 + len(bits) + around)

    def slot(c):
        return xbuf.at[pl.ds(block_len + c * piece, piece)]

    up, down = {"tm": jnp.minimum(k + 1, top)}, {"tm": jnp.maximum(k - 1, 0)}
    sends_up = k < top
    forwards = (k > 0) & (k < top)

    history_copies = [
        remote(xbuf.at[pl.ds(i * piece, piece)], slot(i), hist_s, x_r.at[i], up)
        for i in range(tm_count)
    ]

    def parts(c):
        if c == split:
            return [(0, half, c), (half, piece - half, pieces)]
        return [(0, piece, c)]

    def into(c, src, send, where):
        return [
            remote(
                src.at[pl.ds(first, count)],
                xbuf.at[pl.ds(block_len + c * piece + first, count)],
                send, x_r.at[sem], where,
            )
            for first, count, sem in parts(c)
        ]

    forward_copies = [
        into(i + tm_count, slot(i), fwd_s, up) for i in range(tm_count - 1)
    ]

    def arrivals_from(step, s, target, c):
        copies = into(c, abuf.at[s], arr_s.at[s], {"tm": target})
        return [(k == step, copy) for copy in copies]

    near_copies = arrivals_from(0, 0, 1, tm_count)
    near_copies += arrivals_from(1, 0, 0, 1) + arrivals_from(1, 1, 0, tm_count + 1)
    near_copies += arrivals_from(2, 0, 1, tm_count + 2)
    far_copies, late_copies = [], []
    for i in range(2, tm_count):
        if i > 2:
            far_copies += arrivals_from(i, 0, (i + 1) % 2, i if i % 2 else tm_count + i)
        late_copies += arrivals_from(i, 1, 0, tm_count + i)
    evens, odds = range(2, tm_count, 2), range(3, tm_count, 2)
    relay_copies = {
        i: remote(slot(tm_count + i), slot(i), relay_s, x_r.at[i], {"tm": 0}) for i in evens
    } | {
        i: remote(slot(i), slot(tm_count + i), relay_s, x_r.at[tm_count + i], {"tm": 1})
        for i in odds
    }
    def ext_copy(n):
        source = kflat.at[:, pl.ds((block_len - (n + 1) * piece) * params, piece * params)]
        place = kext.at[:, pl.ds((1 - n) * piece * params, piece * params)]
        return remote(source, place, ext_s, ext_r.at[n], down)

    sends_ext = k > 1

    history_load.wait()

    @pl.when(sends_up)
    def _():
        for copy in history_copies:
            copy.start()

    arrival_load.wait()
    for condition, copy in near_copies:
        pl.when(condition)(copy.start)

    pl.when(k > 0)(lambda: pl.semaphore_wait(ready, 1))
    pl.when(sends_up)(lambda: signal(ready, up))

    for condition, copy in far_copies:
        pl.when(condition)(copy.start)

    if bits[1:]:
        signal(near.at[0], {"par": flipped(1) * 2 + core})

    pltpu.make_async_copy(kflat, kflat, load_s.at[1]).wait()
    pl.when(sends_ext)(ext_copy(0).start)
    pl.when(k == top)(ext_copy(1).start)

    @pl.when(k == 0)
    def _():
        for copy in first_pieces:
            copy.wait()

    pl.when(k == 1)(own_piece.wait)

    for n, d in enumerate(bits[:-1]):
        pl.semaphore_wait(near.at[n], 1)
        if n + 1 < len(bits) - 1:
            signal(near.at[n + 1], {"par": flipped(bits[n + 1]) * 2 + core})

    def taken(unit):
        c = split if unit == pieces else unit
        first, count = [(f, n) for f, n, sem in parts(c) if sem == unit][0]
        place = xbuf.at[pl.ds(block_len + c * piece + first, count)]
        return remote(place, place, hist_s, x_r.at[unit], up)

    def receive(unit):
        c = split if unit == pieces else unit
        i = c % tm_count
        waits = k >= 0
        if i == c:
            waits = (k != 0) if c == 0 or c in odds else waits
        elif i < 2:
            waits = k != i
        elif i % 2 == 0:
            waits = k != 1
        if c == last:
            waits = waits & (k < 2)
        if c == split:
            waits = waits & (k < top)
        pl.when(waits)(taken(unit).wait_recv)

    def relay():
        @pl.when(k == 1)
        def _():
            for i in evens:
                for _, _, unit in parts(tm_count + i):
                    taken(unit).wait_recv()
                relay_copies[i].start()

        @pl.when(k == 0)
        def _():
            for i in odds:
                taken(i).wait_recv()
                relay_copies[i].start()

    def late():
        for condition, copy in late_copies:
            pl.when(condition)(copy.start)

    def span(c):
        return pl.ds(*spans[c])

    def flat_span(c):
        first, count = spans[c]
        return pl.ds(first * rows, count * rows)

    def core_copy(c):
        return remote(
            buf0.at[1 - core, :, span(c)], rcv0.at[:, span(c)], s0, r0.at[c],
            {"par": partner},
        )

    def chip_copy(c, d):
        target = flipped(d)
        return remote(
            mid.at[target, span(c)], mrcv.at[d - 1, span(c)], ms, mr.at[c],
            {"par": target * 2 + core},
        )

    def tm_copy(c, d):
        target = lax.rem(k + d, tm_count)
        place = flat_span(c)
        return remote(
            zbuf.at[target, place], zrcv.at[d - 1, place], zs, zr.at[c],
            {"tm": target},
        )

    def product(r, low, high):
        count = (high - low) * params
        left = xbuf[pl.ds(r + 1 + low, high - low)].reshape(count, fields)
        right = xbuf[pl.ds(r + 2 + low, high - low)].reshape(count, fields)
        both = jnp.concatenate([left, right], 1)
        lags = kflat[:, low * params : high * params]
        return jnp.dot(lags, both, preferred_element_type=F32)

    def hand_over(r, total):
        for side in range(2):
            mine = total[:, side * fields : (side + 1) * fields]
            moved = jnp.concatenate([mine[o * rows : (o + 1) * rows] for o in order], 0)
            moved = moved.astype(BF16)
            for n in range(2 * group):
                buf0[n // group, n % group, r + side] = moved[n * share : (n + 1) * share]

    def compute(c):
        receive(c)
        if c < tm_count - 1:

            @pl.when(forwards & (k < top - 1) if c == tm_count - 2 else forwards)
            def _():
                for copy in forward_copies[c]:
                    copy.start()

        first, count = spans[c]
        for r in range(first, first + count, 2):
            hand_over(r, product(r, 0, block_len))
        core_copy(c).start()

    begin = split * piece
    last_rows = range(begin, steps * block_len, 2)

    def bound(r, c):
        return block_len + c * piece - r - 2

    def early():
        for n, r in enumerate(last_rows):
            acc[n] = product(r, 0, bound(r, split - 1))

    def extra():
        rest = 2 * block_len - wide
        zext[pl.ds(wide - 1 + piece, piece)] = xbuf[pl.ds(rest + piece, piece)]

        @pl.when(k == top - 1)
        def _():
            zext[pl.ds(wide - 1, piece)] = xbuf[pl.ds(rest, piece)]
            ext_copy(1).wait_recv()

        ext_copy(0).wait_recv()
        left = zext[pl.ds(wide - 2, wide)].reshape(wide * params, fields)
        right = zext[pl.ds(wide - 1, wide)].reshape(wide * params, fields)
        both = jnp.concatenate([left, right], 1)
        for n, r in enumerate(last_rows):
            count = (2 * n + 2) * params
            lags = kext[:, wide * params - count :]
            acc[n] = acc[n] + jnp.dot(lags, both[:count], preferred_element_type=F32)

    def middle():
        for n, r in enumerate(last_rows):
            acc[n] = acc[n] + product(r, bound(r, split - 1), bound(r, split))

    def final(c):
        receive((split, pieces, last)[c - split])
        first, count = spans[c]
        for r in range(first, first + count, 2):
            n = (r - begin) // 2
            hand_over(r, acc[n] + product(r, bound(r, split), block_len))
        core_copy(c).start()

    def close(c):
        first, count = spans[c]
        for r in range(first, first + count, 2):
            n = (r - begin) // 2
            hand_over(r, acc[n] + product(r, bound(r, split - 1), bound(r, split) + 1))
        core_copy(c).start()

    def across(c):
        core_copy(c).wait_recv()
        total = buf0[core, :, span(c)].astype(F32) + rcv0[:, span(c)].astype(F32)
        mid[:, span(c)] = total.astype(BF16)
        for d in flips:
            chip_copy(c, d).start()

    def goes_up(d):
        return k + d < tm_count

    def spread(c):
        total = mid[chip, span(c)].astype(F32)
        place = mrcv.at[:, span(c)]
        remote(place, place, ms, mr.at[c], {"par": par}).wait_recv()
        for d in range(1, group):
            total = total + mrcv[d - 1, span(c)].astype(F32)
        for t in range(tm_count):
            mine = [total[g, t * rows : (t + 1) * rows] for g in range(spans[c][1])]
            zbuf[t, flat_span(c)] = jnp.concatenate(mine, 0).astype(BF16)
        for d in range(1, tm_count):
            pl.when(jnp.logical_not(goes_up(d)))(tm_copy(c, d).start)

    def rise(c):
        for d in range(1, tm_count):
            pl.when(goes_up(d))(tm_copy(c, d).start)

    def finish(c):
        place = flat_span(c)
        total = zbuf[k, place].astype(F32)
        taken_parts = zrcv.at[:, place]
        remote(taken_parts, taken_parts, zs, zr.at[c], {"tm": k}).wait_recv()
        for d in range(1, tm_count):
            total = total + zrcv[d - 1, place].astype(F32)
        first, count = spans[c]
        total = total.reshape(count, rows, fields).astype(out_ref.dtype)
        first = first % block_len
        out_ref[spans[c][0] // block_len, first : first + count] = total

    def run(plan):
        for stage, *c in plan:
            stage(*c)

    ends = [(across, split), (across, split + 1), (spread, split - 2)]
    ends += [(rise, c) for c in range(split - 1)]
    ends += [(across, split + 2), (spread, split - 1), (rise, split - 1)]
    for c in range(split, chunks):
        ends += [(spread, c), (rise, c)]

    @pl.when(k == 0)
    def _():
        plan = [(compute, 0), (across, 0), (compute, 1), (relay,), (across, 1), (spread, 0)]
        for c in range(2, split):
            plan.append((compute, c))
            if c > 2:
                plan.append((across, c - 1))
            if c > 3:
                plan.append((spread, c - 3))
        plan += [(early,), (across, split - 1), (spread, split - 3), (middle,), (final, split)]
        plan += [(final, split + 1), (final, split + 2)]
        run(plan + ends)

    def paced(tail):
        plan = []
        for c in range(split):
            plan.append((compute, c))
            if c == split - 2:
                plan.append((early,))
            if c < split - 1:
                plan.append((across, c))
            if c == 0:
                plan.append((relay,))
            if c == 2:
                plan.append((late,))
            if c >= 2:
                plan.append((spread, c - 2))
        run(plan + tail + ends)

    @pl.when(forwards)
    def _():
        tail = [(middle,), (extra,), (across, split - 1)]
        paced(tail + [(final, c) for c in range(split, chunks)])

    @pl.when(k == top)
    def _():
        tail = [(close, split), (across, split - 1), (close, split + 1), (close, split + 2)]
        paced(tail)

    run([(finish, c) for c in range(chunks)])

    def sent(place, sem):
        return remote(place, place, sem, x_r.at[0], up).wait_send

    pl.when(sends_up)(sent(xbuf.at[pl.ds(0, block_len)], hist_s))
    pl.when(forwards)(sent(xbuf.at[pl.ds(0, block_len - wide)], fwd_s))
    pl.when(forwards & (k < top - 1))(sent(xbuf.at[pl.ds(0, piece)], fwd_s))
    sent(abuf.at[0], arr_s.at[0])()
    pl.when(k > 0)(sent(abuf.at[1], arr_s.at[1]))
    for step, those in ((1, evens), (0, odds)):
        if those:
            pl.when(k == step)(sent(xbuf.at[pl.ds(0, len(those) * piece)], relay_s))
    pl.when(sends_ext)(ext_copy(0).wait_send)
    pl.when(k == top)(ext_copy(1).wait_send)
    sent(rcv0, s0)()
    sent(mrcv, ms)()
    sent(zrcv, zs)()


def fused(tm_count, group, kernel, history, arrivals):
    block_len, sensors, params = kernel.shape
    fields = history.shape[2]
    steps = arrivals.shape[0]
    piece = block_len // tm_count
    pieces = steps * tm_count
    outputs = steps * block_len
    share = sensors // (2 * group)
    rows = share // tm_count
    dma = pltpu.SemaphoreType.DMA
    scratch = [
        pltpu.VMEM((sensors, block_len * params), BF16),
        pltpu.VMEM((sensors, 2 * piece * params), BF16),
        pltpu.VMEM(((steps + 1) * block_len, params, fields), BF16),
        pltpu.VMEM((steps, piece, params, fields), BF16),
        pltpu.VMEM((4 * piece - 1, params, fields), BF16),
        pltpu.VMEM((piece, sensors, 2 * fields), F32),
        pltpu.VMEM((2, group, outputs, share, fields), BF16),
        pltpu.VMEM((group, outputs, share, fields), BF16),
        pltpu.VMEM((group, outputs, share, fields), BF16),
        pltpu.VMEM((group - 1, outputs, share, fields), BF16),
        pltpu.VMEM((tm_count, outputs * rows, fields), BF16),
        pltpu.VMEM((tm_count - 1, outputs * rows, fields), BF16),
        dma((3 + steps,)),
        dma(()),
        dma(()),
        dma((2,)),
        dma(()),
        dma(()),
        dma((pieces + 1,)),
        dma((2,)),
        dma(()),
        dma((pieces + 1,)),
        dma(()),
        dma((pieces + 1,)),
        dma(()),
        dma((pieces + 1,)),
        pltpu.SemaphoreType.REGULAR,
        pltpu.SemaphoreType.REGULAR((max(group.bit_length() - 2, 1),)),
    ]
    out_bytes = steps * block_len * rows * fields * 2
    return pl.pallas_call(
        functools.partial(kernel_body, tm_count, group),
        out_shape=pltpu.VMEM((steps, block_len, rows, fields), BF16),
        in_specs=[pl.BlockSpec(memory_space=pltpu.HBM)] * 3,
        out_specs=pl.BlockSpec(memory_space=pltpu.VMEM),
        scratch_shapes=scratch,
        compiler_params=pltpu.CompilerParams(
            collective_id=0, has_side_effects=True, vmem_limit_bytes=VMEM_BYTES - 2 * out_bytes
        ),
    )(kernel, history, arrivals)


def plain(tm_count, kernel, history, arrivals):
    block_len, sensors, params = kernel.shape
    fields = history.shape[2]
    steps = arrivals.shape[0]
    incoming = lax.all_gather(arrivals, "tm", axis=1, tiled=True)
    position = lax.axis_index("tm")
    pairs = [(i, i + 1) for i in range(tm_count - 1)]
    blocks = [history]
    for s in range(steps):
        shifted = lax.ppermute(blocks[-1], "tm", pairs)
        blocks.append(jnp.where(position == 0, incoming[s], shifted))
    window = jnp.concatenate(blocks, 0)
    flat = kernel[::-1].transpose(1, 0, 2).reshape(sensors, block_len * params)

    def one(first):
        part = lax.dynamic_slice_in_dim(window, first, block_len, 0)
        part = part.reshape(block_len * params, fields)
        return jnp.dot(flat, part, preferred_element_type=F32)

    partial = lax.map(one, jnp.arange(steps * block_len, dtype=jnp.int32) + 1)
    partial = partial.reshape(steps, block_len, sensors, fields)
    total = lax.psum_scatter(partial, ("tm", "par"), scatter_dimension=2, tiled=True)
    return total.astype(BF16)


def solution(mesh):
    tm_count, par_count = mesh.shape["tm"], mesh.shape["par"]

    def per_device(kernel, history, arrivals):
        rows = kernel.shape[1] // (tm_count * par_count)
        piece = kernel.shape[0] // tm_count
        fits = rows % 8 == 0 and piece % 4 == 0 and tm_count > 3 and arrivals.shape[0] == 2
        if fits and par_count > 2 and par_count.bit_count() == 1:
            return fused(tm_count, par_count // 2, kernel, history, arrivals)
        return plain(tm_count, kernel, history, arrivals)

    in_specs = (P("tm", None, "par"), P("tm", "par", None), P(None, "tm", "par", None))
    out_specs = P(None, None, ("tm", "par"), None)
    return jax.shard_map(
        per_device, mesh=mesh, in_specs=in_specs, out_specs=out_specs, check_vma=False
    )
```

```python
import functools

import jax
import jax.numpy as jnp
from jax import lax
from jax.experimental import pallas as pl
from jax.experimental.pallas import tpu as pltpu
from jax.sharding import PartitionSpec as P

MESH = pl.DeviceIdType.MESH
F32 = jnp.float32
BF16 = jnp.bfloat16
VMEM_BYTES = 67_043_328
LATE = 2


def kernel_body(
    tm_count, group, k_ref, h_ref, a_ref, out_ref, kflat, kext, xbuf, abuf, zext, acc, buf0, rcv0, mid, mrcv,
    zbuf, zrcv, load_s, hist_s, fwd_s, arr_s, relay_s, ext_s, x_r, ext_r, s0, r0, ms, mr, zs, zr,
    ready, near
):
    block_len, sensors, params = k_ref.shape
    fields = xbuf.shape[2]
    steps = out_ref.shape[0]
    piece = block_len // tm_count
    pieces = steps * tm_count
    last = pieces - 1
    half = piece // 2
    split = last - 1
    spans = [(c * piece, piece) for c in range(split)]
    spans += [(split * piece, half), (split * piece + half, piece - half), (last * piece, piece)]
    chunks = len(spans)
    rows = sensors // (tm_count * group * 2)
    share = sensors // (2 * group)
    k = lax.axis_index("tm")
    par = lax.axis_index("par")
    core, chip = par % 2, par // 2
    partner = par + 1 - 2 * core
    flips = sorted(range(1, group), key=lambda flip: -flip.bit_count())
    top = tm_count - 1

    def flipped(flip):
        target = chip
        for b in range(flip.bit_length()):
            if flip >> b & 1:
                target = target + (1 - 2 * ((chip // (1 << b)) % 2)) * (1 << b)
        return target

    order = [
        (tm * group + q) * 2 + half
        for half in range(2)
        for q in range(group)
        for tm in range(tm_count)
    ]

    def remote(src, dst, send, recv, where):
        return pltpu.make_async_remote_copy(
            src_ref=src, dst_ref=dst, send_sem=send, recv_sem=recv, device_id=where,
            device_id_type=MESH,
        )

    def signal(sem, where):
        pl.semaphore_signal(sem, inc=1, device_id=where, device_id_type=MESH)

    barrier = pltpu.get_barrier_semaphore()
    bits = [1 << b for b in range(group.bit_length() - 1)]
    pl.when(k > 0)(lambda: signal(barrier, {"tm": jnp.maximum(k - 1, 0)}))
    pl.when(k < top)(lambda: signal(barrier, {"tm": jnp.minimum(k + 1, top)}))
    for d in bits:
        signal(barrier, {"par": flipped(d) * 2 + core})
    signal(barrier, {"par": partner})

    history_load = pltpu.make_async_copy(h_ref, xbuf.at[pl.ds(0, block_len)], load_s.at[0])
    kernel_loads = [
        pltpu.make_async_copy(
            k_ref.at[block_len - 1 - j], kflat.at[:, pl.ds(j * params, params)], load_s.at[1]
        )
        for j in range(block_len)
    ]
    first_pieces = []
    for s in range(steps):
        place = xbuf.at[pl.ds(block_len * (s + 1), piece)]
        first_pieces.append(pltpu.make_async_copy(a_ref.at[s], place, load_s.at[2 + s]))
    place = xbuf.at[pl.ds(2 * block_len + piece, piece)]
    own_piece = pltpu.make_async_copy(a_ref.at[0], place, load_s.at[2])

    arrival_load = pltpu.make_async_copy(a_ref, abuf, load_s.at[2 + steps])

    history_load.start()
    arrival_load.start()
    for copy in kernel_loads:
        copy.start()

    @pl.when(k == 0)
    def _():
        for copy in first_pieces:
            copy.start()

    pl.when(k == 1)(own_piece.start)

    wide = 2 * piece
    @pl.when((k > 0) & (k < top - 1))
    def _():
        kext[:, pl.ds(0, piece * params)] = jnp.zeros((sensors, piece * params), BF16)

    @pl.when((k > 1) & (k < top))
    def _():
        tail = xbuf.at[pl.ds(block_len + last * piece, piece)]
        tail[...] = jnp.zeros(tail.shape, BF16)

    @pl.when(k == top)
    def _():
        xbuf[pl.ds(block_len + split * piece, 1)] = jnp.zeros((1, params, fields), BF16)

    zext[pl.ds(0, wide - 1 + piece)] = jnp.zeros((wide - 1 + piece, params, fields), BF16)

    around = (k < top).astype(jnp.int32) + (k > 0).astype(jnp.int32)
    pl.semaphore_wait(barrier, 1 + len(bits) + around)

    def slot(c):
        return xbuf.at[pl.ds(block_len + c * piece, piece)]

    up, down = {"tm": jnp.minimum(k + 1, top)}, {"tm": jnp.maximum(k - 1, 0)}
    sends_up = k < top
    forwards = (k > 0) & (k < top)

    history_copies = [
        remote(xbuf.at[pl.ds(i * piece, piece)], slot(i), hist_s, x_r.at[i], up)
        for i in range(tm_count)
    ]

    def parts(c):
        if c == split:
            return [(0, half, c), (half, piece - half, pieces)]
        return [(0, piece, c)]

    def into(c, src, send, where):
        return [
            remote(
                src.at[pl.ds(first, count)],
                xbuf.at[pl.ds(block_len + c * piece + first, count)],
                send, x_r.at[sem], where,
            )
            for first, count, sem in parts(c)
        ]

    forward_copies = [
        into(i + tm_count, slot(i), fwd_s, up) for i in range(tm_count - 1)
    ]

    def arrivals_from(step, s, target, c):
        copies = into(c, abuf.at[s], arr_s.at[s], {"tm": target})
        return [(k == step, copy) for copy in copies]

    near_copies = arrivals_from(0, 0, 1, tm_count)
    near_copies += arrivals_from(1, 0, 0, 1) + arrivals_from(1, 1, 0, tm_count + 1)
    near_copies += arrivals_from(2, 0, 1, tm_count + 2)
    far_copies, late_copies = [], []
    for i in range(2, tm_count):
        if i > 2:
            far_copies += arrivals_from(i, 0, (i + 1) % 2, i if i % 2 else tm_count + i)
        late_copies += arrivals_from(i, 1, 0, tm_count + i)
    evens, odds = range(2, tm_count, 2), range(3, tm_count, 2)
    relay_copies = {
        i: remote(slot(tm_count + i), slot(i), relay_s, x_r.at[i], {"tm": 0}) for i in evens
    } | {
        i: remote(slot(i), slot(tm_count + i), relay_s, x_r.at[tm_count + i], {"tm": 1})
        for i in odds
    }
    def ext_copy(n, begin=0, count=piece):
        first = (block_len - (n + 1) * piece + begin) * params
        source = kflat.at[:, pl.ds(first, count * params)]
        place = kext.at[:, pl.ds(((1 - n) * piece + begin) * params, count * params)]
        return remote(source, place, ext_s, ext_r.at[n], down)

    sends_ext = k > 1

    history_load.wait()

    @pl.when(sends_up)
    def _():
        for copy in history_copies:
            copy.start()

    arrival_load.wait()
    for condition, copy in near_copies:
        pl.when(condition)(copy.start)

    pltpu.make_async_copy(kflat, kflat, load_s.at[1]).wait()
    pl.when(k == top)(ext_copy(1, 0, 1).start)
    pl.when(k > 0)(lambda: pl.semaphore_wait(ready, 1))
    pl.when(sends_up)(lambda: signal(ready, up))

    for condition, copy in far_copies:
        pl.when(condition)(copy.start)

    if bits[1:]:
        signal(near.at[0], {"par": flipped(1) * 2 + core})

    pl.when(sends_ext)(ext_copy(0).start)
    pl.when(k == top)(ext_copy(1, 1, piece - 1).start)

    @pl.when(k == 0)
    def _():
        for copy in first_pieces:
            copy.wait()

    pl.when(k == 1)(own_piece.wait)

    for n, d in enumerate(bits[:-1]):
        pl.semaphore_wait(near.at[n], 1)
        if n + 1 < len(bits) - 1:
            signal(near.at[n + 1], {"par": flipped(bits[n + 1]) * 2 + core})

    def taken(unit):
        c = split if unit == pieces else unit
        first, count = [(f, n) for f, n, sem in parts(c) if sem == unit][0]
        place = xbuf.at[pl.ds(block_len + c * piece + first, count)]
        return remote(place, place, hist_s, x_r.at[unit], up)

    def receive(unit):
        c = split if unit == pieces else unit
        i = c % tm_count
        waits = k >= 0
        if i == c:
            waits = (k != 0) if c == 0 or c in odds else waits
        elif i < 2:
            waits = k != i
        elif i % 2 == 0:
            waits = k != 1
        if c == last:
            waits = waits & (k < 2)
        if c == split:
            waits = waits & (k < top)
        pl.when(waits)(taken(unit).wait_recv)

    def relay():
        @pl.when(k == 1)
        def _():
            for i in evens:
                for _, _, unit in parts(tm_count + i):
                    taken(unit).wait_recv()
                relay_copies[i].start()

        @pl.when(k == 0)
        def _():
            for i in odds:
                taken(i).wait_recv()
                relay_copies[i].start()

    def late():
        for condition, copy in late_copies:
            pl.when(condition)(copy.start)

    def span(c):
        return pl.ds(*spans[c])

    def flat_span(c):
        first, count = spans[c]
        return pl.ds(first * rows, count * rows)

    def core_copy(c):
        return remote(
            buf0.at[1 - core, :, span(c)], rcv0.at[:, span(c)], s0, r0.at[c],
            {"par": partner},
        )

    def chip_copy(c, d):
        target = flipped(d)
        return remote(
            mid.at[target, span(c)], mrcv.at[d - 1, span(c)], ms, mr.at[c],
            {"par": target * 2 + core},
        )

    def tm_copy(c, d):
        target = lax.rem(k + d, tm_count)
        place = flat_span(c)
        return remote(
            zbuf.at[target, place], zrcv.at[d - 1, place], zs, zr.at[tm_sem(c)],
            {"tm": target},
        )

    def tm_sem(c):
        return max(c - (split - 2), 0)

    def product(r, low, high):
        count = (high - low) * params
        left = xbuf[pl.ds(r + 1 + low, high - low)].reshape(count, fields)
        right = xbuf[pl.ds(r + 2 + low, high - low)].reshape(count, fields)
        both = jnp.concatenate([left, right], 1)
        lags = kflat[:, low * params : high * params]
        return jnp.dot(lags, both, preferred_element_type=F32)

    def hand_over(r, total):
        for side in range(2):
            mine = total[:, side * fields : (side + 1) * fields]
            moved = jnp.concatenate([mine[o * rows : (o + 1) * rows] for o in order], 0)
            moved = moved.astype(BF16)
            for n in range(2 * group):
                buf0[n // group, n % group, r + side] = moved[n * share : (n + 1) * share]

    def compute(c):
        receive(c)
        if c < tm_count - 1:

            @pl.when(forwards & (k < top - 1) if c == tm_count - 2 else forwards)
            def _():
                for copy in forward_copies[c]:
                    copy.start()

        first, count = spans[c]
        for r in range(first, first + count, 2):
            hand_over(r, product(r, 0, block_len))
        core_copy(c).start()

    begin = split * piece
    last_rows = range(begin, steps * block_len, 2)

    def bound(r, c):
        return block_len + c * piece - r - 2

    def early():
        for n, r in enumerate(last_rows):
            acc[n] = product(r, 0, bound(r, split - 1))

    def extra():
        rest = 2 * block_len - wide
        zext[pl.ds(wide - 1 + piece, piece)] = xbuf[pl.ds(rest + piece, piece)]

        @pl.when(k == top - 1)
        def _():
            zext[pl.ds(wide - 1, piece)] = xbuf[pl.ds(rest, piece)]
            ext_copy(1).wait_recv()

        ext_copy(0).wait_recv()
        left = zext[pl.ds(wide - 2, wide)].reshape(wide * params, fields)
        right = zext[pl.ds(wide - 1, wide)].reshape(wide * params, fields)
        both = jnp.concatenate([left, right], 1)
        for n, r in enumerate(last_rows):
            count = (2 * n + 2) * params
            lags = kext[:, wide * params - count :]
            acc[n] = acc[n] + jnp.dot(lags, both[:count], preferred_element_type=F32)

    def middle():
        for n, r in enumerate(last_rows):
            acc[n] = acc[n] + product(r, bound(r, split - 1), bound(r, split))

    def final(c):
        receive((split, pieces, last)[c - split])
        first, count = spans[c]
        for r in range(first, first + count, 2):
            n = (r - begin) // 2
            hand_over(r, acc[n] + product(r, bound(r, split), block_len))
        core_copy(c).start()

    def close(c):
        first, count = spans[c]
        for r in range(first, first + count, 2):
            n = (r - begin) // 2
            hand_over(r, acc[n] + product(r, bound(r, split - 1), bound(r, split) + 1))
        core_copy(c).start()

    def across(c):
        core_copy(c).wait_recv()
        total = buf0[core, :, span(c)].astype(F32) + rcv0[:, span(c)].astype(F32)
        mid[:, span(c)] = total.astype(BF16)
        for d in flips:
            chip_copy(c, d).start()

    def goes_up(d):
        return k + d < tm_count

    def spread(c):
        total = mid[chip, span(c)].astype(F32)
        place = mrcv.at[:, span(c)]
        remote(place, place, ms, mr.at[c], {"par": par}).wait_recv()
        for d in range(1, group):
            total = total + mrcv[d - 1, span(c)].astype(F32)
        for t in range(tm_count):
            mine = [total[g, t * rows : (t + 1) * rows] for g in range(spans[c][1])]
            zbuf[t, flat_span(c)] = jnp.concatenate(mine, 0).astype(BF16)
        for d in range(1, tm_count):
            pl.when(jnp.logical_not(goes_up(d)))(tm_copy(c, d).start)

    def rise(c):
        for d in range(1, tm_count):
            pl.when(goes_up(d))(tm_copy(c, d).start)

    def finish(c):
        place = flat_span(c)
        total = zbuf[k, place].astype(F32)
        if tm_sem(c):
            taken_parts = zrcv.at[:, place]
        else:
            taken_parts = zrcv.at[:, pl.ds(0, (split - 1) * piece * rows)]
        if tm_sem(c) or c == 0:
            remote(taken_parts, taken_parts, zs, zr.at[tm_sem(c)], {"tm": k}).wait_recv()
        for d in range(1, tm_count):
            total = total + zrcv[d - 1, place].astype(F32)
        first, count = spans[c]
        total = total.reshape(count, rows, fields).astype(out_ref.dtype)
        first = first % block_len
        out_ref[spans[c][0] // block_len, first : first + count] = total

    def across_on(which, c):
        pl.when(core == which)(lambda: across(c))

    def run(plan):
        for stage, *c in plan:
            stage(*c)

    ends = [(across, split), (across, split + 1), (spread, split - 2)]
    ends += [(rise, c) for c in range(split - 1)]
    ends += [(across, split + 2), (spread, split - 1), (rise, split - 1)]
    for c in range(split, chunks):
        ends += [(spread, c), (rise, c)]

    @pl.when(k == 0)
    def _():
        plan = [(compute, 0), (across, 0), (compute, 1), (relay,), (across, 1), (spread, 0)]
        for c in range(2, split):
            plan.append((compute, c))
            if c > 2:
                plan.append((across, c - 1))
            if c > 3:
                plan.append((spread, c - 3))
        plan += [(early,), (across, split - 1), (spread, split - 3), (middle,), (final, split)]
        plan += [(final, split + 1), (final, split + 2)]
        run(plan + ends)

    def paced(tail):
        plan = []
        for c in range(split - 1):
            plan.append((compute, c))
            if c == split - 2:
                plan.append((early,))
            else:
                plan.append((across, c))
            if c == 0:
                plan.append((relay,))
            if c == 2:
                plan.append((late,))
            if 2 <= c < split - 2:
                plan.append((spread, c - 2))
        plan += [(across_on, 0, split - 2), (spread, split - 4)]
        run(plan + tail + ends)

    @pl.when(forwards)
    def _():
        tail = [(extra,), (compute, split - 1), (across_on, 1, split - 2), (spread, split - 3)]
        tail += [(across_on, 0, split - 1), (middle,), (final, split), (across_on, 1, split - 1)]
        paced(tail + [(final, c) for c in range(split + 1, chunks)])

    @pl.when(k == top)
    def _():
        tail = [(compute, split - 1), (across_on, 1, split - 2), (spread, split - 3)]
        tail += [(close, split), (across, split - 1), (close, split + 1), (close, split + 2)]
        paced(tail)

    run([(finish, c) for c in range(chunks)])

    def sent(place, sem):
        return remote(place, place, sem, x_r.at[0], up).wait_send

    pl.when(sends_up)(sent(xbuf.at[pl.ds(0, block_len)], hist_s))
    pl.when(forwards)(sent(xbuf.at[pl.ds(0, block_len - wide)], fwd_s))
    pl.when(forwards & (k < top - 1))(sent(xbuf.at[pl.ds(0, piece)], fwd_s))
    sent(abuf.at[0], arr_s.at[0])()
    pl.when(k > 0)(sent(abuf.at[1], arr_s.at[1]))
    for step, those in ((1, evens), (0, odds)):
        if those:
            pl.when(k == step)(sent(xbuf.at[pl.ds(0, len(those) * piece)], relay_s))
    pl.when(sends_ext)(ext_copy(0).wait_send)
    pl.when(k == top)(ext_copy(1).wait_send)
    sent(rcv0, s0)()
    sent(mrcv, ms)()
    sent(zrcv, zs)()


def fused(tm_count, group, kernel, history, arrivals):
    block_len, sensors, params = kernel.shape
    fields = history.shape[2]
    steps = arrivals.shape[0]
    piece = block_len // tm_count
    pieces = steps * tm_count
    outputs = steps * block_len
    share = sensors // (2 * group)
    rows = share // tm_count
    dma = pltpu.SemaphoreType.DMA
    scratch = [
        pltpu.VMEM((sensors, block_len * params), BF16),
        pltpu.VMEM((sensors, 2 * piece * params), BF16),
        pltpu.VMEM(((steps + 1) * block_len, params, fields), BF16),
        pltpu.VMEM((steps, piece, params, fields), BF16),
        pltpu.VMEM((4 * piece - 1, params, fields), BF16),
        pltpu.VMEM((piece, sensors, 2 * fields), F32),
        pltpu.VMEM((2, group, outputs, share, fields), BF16),
        pltpu.VMEM((group, outputs, share, fields), BF16),
        pltpu.VMEM((group, outputs, share, fields), BF16),
        pltpu.VMEM((group - 1, outputs, share, fields), BF16),
        pltpu.VMEM((tm_count, outputs * rows, fields), BF16),
        pltpu.VMEM((tm_count - 1, outputs * rows, fields), BF16),
        dma((3 + steps,)),
        dma(()),
        dma(()),
        dma((2,)),
        dma(()),
        dma(()),
        dma((pieces + 1,)),
        dma((2,)),
        dma(()),
        dma((pieces + 1,)),
        dma(()),
        dma((pieces + 1,)),
        dma(()),
        dma((5,)),
        pltpu.SemaphoreType.REGULAR,
        pltpu.SemaphoreType.REGULAR((max(group.bit_length() - 2, 1),)),
    ]
    out_bytes = steps * block_len * rows * fields * 2
    return pl.pallas_call(
        functools.partial(kernel_body, tm_count, group),
        out_shape=pltpu.VMEM((steps, block_len, rows, fields), BF16),
        in_specs=[pl.BlockSpec(memory_space=pltpu.HBM)] * 3,
        out_specs=pl.BlockSpec(memory_space=pltpu.VMEM),
        scratch_shapes=scratch,
        compiler_params=pltpu.CompilerParams(
            collective_id=0, has_side_effects=True, vmem_limit_bytes=VMEM_BYTES - 2 * out_bytes
        ),
    )(kernel, history, arrivals)


def plain(tm_count, kernel, history, arrivals):
    block_len, sensors, params = kernel.shape
    fields = history.shape[2]
    steps = arrivals.shape[0]
    incoming = lax.all_gather(arrivals, "tm", axis=1, tiled=True)
    position = lax.axis_index("tm")
    pairs = [(i, i + 1) for i in range(tm_count - 1)]
    blocks = [history]
    for s in range(steps):
        shifted = lax.ppermute(blocks[-1], "tm", pairs)
        blocks.append(jnp.where(position == 0, incoming[s], shifted))
    window = jnp.concatenate(blocks, 0)
    flat = kernel[::-1].transpose(1, 0, 2).reshape(sensors, block_len * params)

    def one(first):
        part = lax.dynamic_slice_in_dim(window, first, block_len, 0)
        part = part.reshape(block_len * params, fields)
        return jnp.dot(flat, part, preferred_element_type=F32)

    partial = lax.map(one, jnp.arange(steps * block_len, dtype=jnp.int32) + 1)
    partial = partial.reshape(steps, block_len, sensors, fields)
    total = lax.psum_scatter(partial, ("tm", "par"), scatter_dimension=2, tiled=True)
    return total.astype(BF16)


def solution(mesh):
    tm_count, par_count = mesh.shape["tm"], mesh.shape["par"]

    def per_device(kernel, history, arrivals):
        rows = kernel.shape[1] // (tm_count * par_count)
        piece = kernel.shape[0] // tm_count
        fits = rows % 8 == 0 and piece % 4 == 0 and tm_count > 3 and arrivals.shape[0] == 2
        if fits and par_count > 2 and par_count.bit_count() == 1:
            return fused(tm_count, par_count // 2, kernel, history, arrivals)
        return plain(tm_count, kernel, history, arrivals)

    in_specs = (P("tm", None, "par"), P("tm", "par", None), P(None, "tm", "par", None))
    out_specs = P(None, None, ("tm", "par"), None)
    return jax.shard_map(
        per_device, mesh=mesh, in_specs=in_specs, out_specs=out_specs, check_vma=False
    )
```

```python
import functools

import jax
import jax.numpy as jnp
from jax import lax
from jax.experimental import pallas as pl
from jax.experimental.pallas import tpu as pltpu
from jax.sharding import PartitionSpec as P

MESH = pl.DeviceIdType.MESH
F32 = jnp.float32
BF16 = jnp.bfloat16
VMEM_BYTES = 67_043_328
LATE = 2


def kernel_body(
    tm_count, group, k_ref, h_ref, a_ref, out_ref, kflat, kext, xbuf, abuf, zext, acc, buf0, rcv0, mid, mrcv,
    zbuf, zrcv, load_s, hist_s, fwd_s, arr_s, relay_s, ext_s, x_r, ext_r, s0, r0, ms, mr, zs, zr,
    ready, near
):
    block_len, sensors, params = k_ref.shape
    fields = xbuf.shape[2]
    steps = out_ref.shape[0]
    piece = block_len // tm_count
    pieces = steps * tm_count
    last = pieces - 1
    half = piece // 2
    split = last - 1
    spans = [(c * piece, piece) for c in range(split)]
    spans += [(split * piece, half), (split * piece + half, piece - half), (last * piece, piece)]
    chunks = len(spans)
    rows = sensors // (tm_count * group * 2)
    share = sensors // (2 * group)
    k = lax.axis_index("tm")
    par = lax.axis_index("par")
    core, chip = par % 2, par // 2
    partner = par + 1 - 2 * core
    flips = sorted(range(1, group), key=lambda flip: -flip.bit_count())
    top = tm_count - 1

    def flipped(flip):
        target = chip
        for b in range(flip.bit_length()):
            if flip >> b & 1:
                target = target + (1 - 2 * ((chip // (1 << b)) % 2)) * (1 << b)
        return target

    order = [
        (tm * group + q) * 2 + half
        for half in range(2)
        for q in range(group)
        for tm in range(tm_count)
    ]

    def remote(src, dst, send, recv, where):
        return pltpu.make_async_remote_copy(
            src_ref=src, dst_ref=dst, send_sem=send, recv_sem=recv, device_id=where,
            device_id_type=MESH,
        )

    def signal(sem, where):
        pl.semaphore_signal(sem, inc=1, device_id=where, device_id_type=MESH)

    barrier = pltpu.get_barrier_semaphore()
    bits = [1 << b for b in range(group.bit_length() - 1)]
    pl.when(k > 0)(lambda: signal(barrier, {"tm": jnp.maximum(k - 1, 0)}))
    pl.when(k < top)(lambda: signal(barrier, {"tm": jnp.minimum(k + 1, top)}))
    for d in bits:
        signal(barrier, {"par": flipped(d) * 2 + core})
    signal(barrier, {"par": partner})

    history_load = pltpu.make_async_copy(h_ref, xbuf.at[pl.ds(0, block_len)], load_s.at[0])
    kernel_loads = [
        pltpu.make_async_copy(
            k_ref.at[block_len - 1 - j], kflat.at[:, pl.ds(j * params, params)], load_s.at[1]
        )
        for j in range(block_len)
    ]
    first_pieces = []
    for s in range(steps):
        place = xbuf.at[pl.ds(block_len * (s + 1), piece)]
        first_pieces.append(pltpu.make_async_copy(a_ref.at[s], place, load_s.at[2 + s]))
    place = xbuf.at[pl.ds(2 * block_len + piece, piece)]
    own_piece = pltpu.make_async_copy(a_ref.at[0], place, load_s.at[2])

    arrival_load = pltpu.make_async_copy(a_ref, abuf, load_s.at[2 + steps])

    history_load.start()
    arrival_load.start()
    for copy in kernel_loads:
        copy.start()

    @pl.when(k == 0)
    def _():
        for copy in first_pieces:
            copy.start()

    pl.when(k == 1)(own_piece.start)

    wide = 2 * piece
    @pl.when((k > 0) & (k < top - 1))
    def _():
        kext[:, pl.ds(0, piece * params)] = jnp.zeros((sensors, piece * params), BF16)

    @pl.when((k > 1) & (k < top))
    def _():
        tail = xbuf.at[pl.ds(block_len + last * piece, piece)]
        tail[...] = jnp.zeros(tail.shape, BF16)

    @pl.when(k == top)
    def _():
        xbuf[pl.ds(block_len + split * piece, 1)] = jnp.zeros((1, params, fields), BF16)

    zext[pl.ds(0, wide - 1 + piece)] = jnp.zeros((wide - 1 + piece, params, fields), BF16)

    around = (k < top).astype(jnp.int32) + (k > 0).astype(jnp.int32)
    pl.semaphore_wait(barrier, 1 + len(bits) + around)

    def slot(c):
        return xbuf.at[pl.ds(block_len + c * piece, piece)]

    up, down = {"tm": jnp.minimum(k + 1, top)}, {"tm": jnp.maximum(k - 1, 0)}
    sends_up = k < top
    forwards = (k > 0) & (k < top)

    history_copies = [
        remote(xbuf.at[pl.ds(i * piece, piece)], slot(i), hist_s, x_r.at[i], up)
        for i in range(tm_count)
    ]

    def parts(c):
        if c == split:
            return [(0, half, c), (half, piece - half, pieces)]
        return [(0, piece, c)]

    def into(c, src, send, where):
        return [
            remote(
                src.at[pl.ds(first, count)],
                xbuf.at[pl.ds(block_len + c * piece + first, count)],
                send, x_r.at[sem], where,
            )
            for first, count, sem in parts(c)
        ]

    forward_copies = [
        into(i + tm_count, slot(i), fwd_s, up) for i in range(tm_count - 1)
    ]

    def arrivals_from(step, s, target, c):
        copies = into(c, abuf.at[s], arr_s.at[s], {"tm": target})
        return [(k == step, copy) for copy in copies]

    near_copies = arrivals_from(0, 0, 1, tm_count)
    near_copies += arrivals_from(1, 0, 0, 1) + arrivals_from(1, 1, 0, tm_count + 1)
    near_copies += arrivals_from(2, 0, 1, tm_count + 2)
    far_copies, late_copies = [], []
    for i in range(2, tm_count):
        if i > 2:
            far_copies += arrivals_from(i, 0, (i + 1) % 2, i if i % 2 else tm_count + i)
        late_copies += arrivals_from(i, 1, 0, tm_count + i)
    evens, odds = range(2, tm_count, 2), range(3, tm_count, 2)
    relay_copies = {
        i: remote(slot(tm_count + i), slot(i), relay_s, x_r.at[i], {"tm": 0}) for i in evens
    } | {
        i: remote(slot(i), slot(tm_count + i), relay_s, x_r.at[tm_count + i], {"tm": 1})
        for i in odds
    }
    def ext_copy(n, begin=0, count=piece):
        first = (block_len - (n + 1) * piece + begin) * params
        source = kflat.at[:, pl.ds(first, count * params)]
        place = kext.at[:, pl.ds(((1 - n) * piece + begin) * params, count * params)]
        return remote(source, place, ext_s, ext_r.at[n], down)

    sends_ext = k > 1

    history_load.wait()

    @pl.when(sends_up)
    def _():
        for copy in history_copies:
            copy.start()

    arrival_load.wait()
    for condition, copy in near_copies:
        pl.when(condition)(copy.start)

    pltpu.make_async_copy(kflat, kflat, load_s.at[1]).wait()
    pl.when(k == top)(ext_copy(1, 0, 1).start)
    pl.when(k > 0)(lambda: pl.semaphore_wait(ready, 1))
    pl.when(sends_up)(lambda: signal(ready, up))

    for condition, copy in far_copies:
        pl.when(condition)(copy.start)

    if bits[1:]:
        signal(near.at[0], {"par": flipped(1) * 2 + core})

    pl.when(sends_ext)(ext_copy(0).start)
    pl.when(k == top)(ext_copy(1, 1, piece - 1).start)

    @pl.when(k == 0)
    def _():
        for copy in first_pieces:
            copy.wait()

    pl.when(k == 1)(own_piece.wait)

    for n, d in enumerate(bits[:-1]):
        pl.semaphore_wait(near.at[n], 1)
        if n + 1 < len(bits) - 1:
            signal(near.at[n + 1], {"par": flipped(bits[n + 1]) * 2 + core})

    def taken(unit):
        c = split if unit == pieces else unit
        first, count = [(f, n) for f, n, sem in parts(c) if sem == unit][0]
        place = xbuf.at[pl.ds(block_len + c * piece + first, count)]
        return remote(place, place, hist_s, x_r.at[unit], up)

    def receive(unit):
        c = split if unit == pieces else unit
        i = c % tm_count
        waits = k >= 0
        if i == c:
            waits = (k != 0) if c == 0 or c in odds else waits
        elif i < 2:
            waits = k != i
        elif i % 2 == 0:
            waits = k != 1
        if c == last:
            waits = waits & (k < 2)
        if c == split:
            waits = waits & (k < top)
        pl.when(waits)(taken(unit).wait_recv)

    def relay():
        @pl.when(k == 1)
        def _():
            for i in evens:
                for _, _, unit in parts(tm_count + i):
                    taken(unit).wait_recv()
                relay_copies[i].start()

        @pl.when(k == 0)
        def _():
            for i in odds:
                taken(i).wait_recv()
                relay_copies[i].start()

    def late():
        for condition, copy in late_copies:
            pl.when(condition)(copy.start)

    def span(c):
        return pl.ds(*spans[c])

    def flat_span(c):
        first, count = spans[c]
        return pl.ds(first * rows, count * rows)

    def core_copy(c):
        return remote(
            buf0.at[1 - core, :, span(c)], rcv0.at[:, span(c)], s0, r0.at[c],
            {"par": partner},
        )

    def chip_copy(c, d):
        target = flipped(d)
        return remote(
            mid.at[target, span(c)], mrcv.at[d - 1, span(c)], ms, mr.at[c],
            {"par": target * 2 + core},
        )

    def tm_copy(c, d):
        target = lax.rem(k + d, tm_count)
        place = flat_span(c)
        return remote(
            zbuf.at[target, place], zrcv.at[d - 1, place], zs, zr.at[tm_sem(c)],
            {"tm": target},
        )

    def tm_sem(c):
        return max(c - (split - 2), 0)

    def product(r, low, high):
        count = (high - low) * params
        left = xbuf[pl.ds(r + 1 + low, high - low)].reshape(count, fields)
        right = xbuf[pl.ds(r + 2 + low, high - low)].reshape(count, fields)
        both = jnp.concatenate([left, right], 1)
        lags = kflat[:, low * params : high * params]
        return jnp.dot(lags, both, preferred_element_type=F32)

    def hand_over(r, total):
        for side in range(2):
            mine = total[:, side * fields : (side + 1) * fields]
            moved = jnp.concatenate([mine[o * rows : (o + 1) * rows] for o in order], 0)
            moved = moved.astype(BF16)
            for n in range(2 * group):
                buf0[n // group, n % group, r + side] = moved[n * share : (n + 1) * share]

    def compute(c):
        receive(c)
        if c < tm_count - 1:

            @pl.when(forwards & (k < top - 1) if c == tm_count - 2 else forwards)
            def _():
                for copy in forward_copies[c]:
                    copy.start()

        first, count = spans[c]
        for r in range(first, first + count, 2):
            hand_over(r, product(r, 0, block_len))
        core_copy(c).start()

    begin = (split - 1) * piece
    last_rows = list(enumerate(range(begin, steps * block_len, 2)))
    latest = [(n, r) for n, r in last_rows if r >= split * piece]

    def bound(r, c):
        return block_len + c * piece - r - 2

    def early():
        for n, r in last_rows:
            acc[n] = product(r, 0, bound(r, split - 1))

    def extra():
        rest = 2 * block_len - wide
        zext[pl.ds(wide - 1 + piece, piece)] = xbuf[pl.ds(rest + piece, piece)]

        @pl.when(k == top - 1)
        def _():
            zext[pl.ds(wide - 1, piece)] = xbuf[pl.ds(rest, piece)]
            ext_copy(1).wait_recv()

        ext_copy(0).wait_recv()
        left = zext[pl.ds(wide - 2, wide)].reshape(wide * params, fields)
        right = zext[pl.ds(wide - 1, wide)].reshape(wide * params, fields)
        both = jnp.concatenate([left, right], 1)
        for n, r in latest:
            count = (r + 2 - split * piece) * params
            lags = kext[:, wide * params - count :]
            acc[n] = acc[n] + jnp.dot(lags, both[:count], preferred_element_type=F32)

    def middle():
        for n, r in latest:
            acc[n] = acc[n] + product(r, bound(r, split - 1), bound(r, split))

    def final(c):
        receive((split - 1, split, pieces, last)[c - split + 1])
        first, count = spans[c]
        for r in range(first, first + count, 2):
            n = (r - begin) // 2
            hand_over(r, acc[n] + product(r, bound(r, min(c, split)), block_len))
        core_copy(c).start()

    def close(c):
        first, count = spans[c]
        for r in range(first, first + count, 2):
            n = (r - begin) // 2
            hand_over(r, acc[n] + product(r, bound(r, split - 1), bound(r, split) + 1))
        core_copy(c).start()

    def across(c):
        core_copy(c).wait_recv()
        total = buf0[core, :, span(c)].astype(F32) + rcv0[:, span(c)].astype(F32)
        mid[:, span(c)] = total.astype(BF16)
        for d in flips:
            chip_copy(c, d).start()

    def goes_up(d):
        return k + d < tm_count

    def spread(c):
        total = mid[chip, span(c)].astype(F32)
        place = mrcv.at[:, span(c)]
        remote(place, place, ms, mr.at[c], {"par": par}).wait_recv()
        for d in range(1, group):
            total = total + mrcv[d - 1, span(c)].astype(F32)
        for t in range(tm_count):
            mine = [total[g, t * rows : (t + 1) * rows] for g in range(spans[c][1])]
            zbuf[t, flat_span(c)] = jnp.concatenate(mine, 0).astype(BF16)
        for d in range(1, tm_count):
            pl.when(jnp.logical_not(goes_up(d)))(tm_copy(c, d).start)

    def rise(c):
        for d in range(1, tm_count):
            pl.when(goes_up(d))(tm_copy(c, d).start)

    def finish(c):
        place = flat_span(c)
        total = zbuf[k, place].astype(F32)
        if tm_sem(c):
            taken_parts = zrcv.at[:, place]
        else:
            taken_parts = zrcv.at[:, pl.ds(0, (split - 1) * piece * rows)]
        if tm_sem(c) or c == 0:
            remote(taken_parts, taken_parts, zs, zr.at[tm_sem(c)], {"tm": k}).wait_recv()
        for d in range(1, tm_count):
            total = total + zrcv[d - 1, place].astype(F32)
        first, count = spans[c]
        total = total.reshape(count, rows, fields).astype(out_ref.dtype)
        first = first % block_len
        out_ref[spans[c][0] // block_len, first : first + count] = total

    def across_on(which, c):
        pl.when(core == which)(lambda: across(c))

    def run(plan):
        for stage, *c in plan:
            stage(*c)

    ends = [(across, split + 1), (across, split + 2), (spread, split - 2)]
    ends += [(rise, c) for c in range(split - 1)]
    ends += [(spread, split - 1), (rise, split - 1)]
    for c in range(split, chunks):
        ends += [(spread, c), (rise, c)]

    @pl.when(k == 0)
    def _():
        plan = [(compute, 0), (across, 0), (compute, 1), (relay,), (across, 1), (spread, 0)]
        for c in range(2, split - 1):
            plan.append((compute, c))
            if c > 2:
                plan.append((across, c - 1))
            if c > 3:
                plan.append((spread, c - 3))
        plan += [(early,), (final, split - 1), (across, split - 2), (spread, split - 4)]
        plan += [(across, split - 1), (spread, split - 3), (middle,)]
        plan += [(final, c) for c in range(split, chunks)]
        run(plan + [(across, split)] + ends)

    def paced(tail):
        plan = []
        for c in range(split - 1):
            plan.append((compute, c))
            if c == split - 2:
                plan.append((early,))
            else:
                plan.append((across, c))
            if c == 0:
                plan.append((relay,))
            if c == 2:
                plan.append((late,))
            if 2 <= c < split - 2:
                plan.append((spread, c - 2))
        plan += [(across_on, 0, split - 2), (spread, split - 4)]
        run(plan + tail + ends)

    @pl.when(forwards)
    def _():
        tail = [(extra,), (final, split - 1), (across_on, 1, split - 2), (spread, split - 3)]
        tail += [(across_on, 0, split - 1), (middle,), (final, split), (across_on, 0, split)]
        tail += [(across_on, 1, split - 1), (final, split + 1), (final, split + 2)]
        paced(tail + [(across_on, 1, split)])

    @pl.when(k == top)
    def _():
        tail = [(final, split - 1), (across_on, 1, split - 2), (spread, split - 3), (close, split)]
        tail += [(across, split - 1), (close, split + 1), (close, split + 2), (across, split)]
        paced(tail)

    run([(finish, c) for c in range(chunks)])

    def sent(place, sem):
        return remote(place, place, sem, x_r.at[0], up).wait_send

    pl.when(sends_up)(sent(xbuf.at[pl.ds(0, block_len)], hist_s))
    pl.when(forwards)(sent(xbuf.at[pl.ds(0, block_len - wide)], fwd_s))
    pl.when(forwards & (k < top - 1))(sent(xbuf.at[pl.ds(0, piece)], fwd_s))
    sent(abuf.at[0], arr_s.at[0])()
    pl.when(k > 0)(sent(abuf.at[1], arr_s.at[1]))
    for step, those in ((1, evens), (0, odds)):
        if those:
            pl.when(k == step)(sent(xbuf.at[pl.ds(0, len(those) * piece)], relay_s))
    pl.when(sends_ext)(ext_copy(0).wait_send)
    pl.when(k == top)(ext_copy(1).wait_send)
    sent(rcv0, s0)()
    sent(mrcv, ms)()
    sent(zrcv, zs)()


def fused(tm_count, group, kernel, history, arrivals):
    block_len, sensors, params = kernel.shape
    fields = history.shape[2]
    steps = arrivals.shape[0]
    piece = block_len // tm_count
    pieces = steps * tm_count
    outputs = steps * block_len
    share = sensors // (2 * group)
    rows = share // tm_count
    dma = pltpu.SemaphoreType.DMA
    scratch = [
        pltpu.VMEM((sensors, block_len * params), BF16),
        pltpu.VMEM((sensors, 2 * piece * params), BF16),
        pltpu.VMEM(((steps + 1) * block_len, params, fields), BF16),
        pltpu.VMEM((steps, piece, params, fields), BF16),
        pltpu.VMEM((4 * piece - 1, params, fields), BF16),
        pltpu.VMEM((piece + piece // 2, sensors, 2 * fields), F32),
        pltpu.VMEM((2, group, outputs, share, fields), BF16),
        pltpu.VMEM((group, outputs, share, fields), BF16),
        pltpu.VMEM((group, outputs, share, fields), BF16),
        pltpu.VMEM((group - 1, outputs, share, fields), BF16),
        pltpu.VMEM((tm_count, outputs * rows, fields), BF16),
        pltpu.VMEM((tm_count - 1, outputs * rows, fields), BF16),
        dma((3 + steps,)),
        dma(()),
        dma(()),
        dma((2,)),
        dma(()),
        dma(()),
        dma((pieces + 1,)),
        dma((2,)),
        dma(()),
        dma((pieces + 1,)),
        dma(()),
        dma((pieces + 1,)),
        dma(()),
        dma((5,)),
        pltpu.SemaphoreType.REGULAR,
        pltpu.SemaphoreType.REGULAR((max(group.bit_length() - 2, 1),)),
    ]
    out_bytes = steps * block_len * rows * fields * 2
    return pl.pallas_call(
        functools.partial(kernel_body, tm_count, group),
        out_shape=pltpu.VMEM((steps, block_len, rows, fields), BF16),
        in_specs=[pl.BlockSpec(memory_space=pltpu.HBM)] * 3,
        out_specs=pl.BlockSpec(memory_space=pltpu.VMEM),
        scratch_shapes=scratch,
        compiler_params=pltpu.CompilerParams(
            collective_id=0, has_side_effects=True, vmem_limit_bytes=VMEM_BYTES - 2 * out_bytes
        ),
    )(kernel, history, arrivals)


def plain(tm_count, kernel, history, arrivals):
    block_len, sensors, params = kernel.shape
    fields = history.shape[2]
    steps = arrivals.shape[0]
    incoming = lax.all_gather(arrivals, "tm", axis=1, tiled=True)
    position = lax.axis_index("tm")
    pairs = [(i, i + 1) for i in range(tm_count - 1)]
    blocks = [history]
    for s in range(steps):
        shifted = lax.ppermute(blocks[-1], "tm", pairs)
        blocks.append(jnp.where(position == 0, incoming[s], shifted))
    window = jnp.concatenate(blocks, 0)
    flat = kernel[::-1].transpose(1, 0, 2).reshape(sensors, block_len * params)

    def one(first):
        part = lax.dynamic_slice_in_dim(window, first, block_len, 0)
        part = part.reshape(block_len * params, fields)
        return jnp.dot(flat, part, preferred_element_type=F32)

    partial = lax.map(one, jnp.arange(steps * block_len, dtype=jnp.int32) + 1)
    partial = partial.reshape(steps, block_len, sensors, fields)
    total = lax.psum_scatter(partial, ("tm", "par"), scatter_dimension=2, tiled=True)
    return total.astype(BF16)


def solution(mesh):
    tm_count, par_count = mesh.shape["tm"], mesh.shape["par"]

    def per_device(kernel, history, arrivals):
        rows = kernel.shape[1] // (tm_count * par_count)
        piece = kernel.shape[0] // tm_count
        fits = rows % 8 == 0 and piece % 4 == 0 and tm_count > 3 and arrivals.shape[0] == 2
        if fits and par_count > 2 and par_count.bit_count() == 1:
            return fused(tm_count, par_count // 2, kernel, history, arrivals)
        return plain(tm_count, kernel, history, arrivals)

    in_specs = (P("tm", None, "par"), P("tm", "par", None), P(None, "tm", "par", None))
    out_specs = P(None, None, ("tm", "par"), None)
    return jax.shard_map(
        per_device, mesh=mesh, in_specs=in_specs, out_specs=out_specs, check_vma=False
    )
```

```python
import functools

import jax
import jax.numpy as jnp
from jax import lax
from jax.experimental import pallas as pl
from jax.experimental.pallas import tpu as pltpu
from jax.sharding import PartitionSpec as P

MESH = pl.DeviceIdType.MESH
F32 = jnp.float32
BF16 = jnp.bfloat16
VMEM_BYTES = 67_043_328
LATE = 2


def kernel_body(
    tm_count, group, k_ref, h_ref, a_ref, out_ref, kflat, kext, xbuf, abuf, zext, acc, buf0, rcv0, mid, mrcv,
    zbuf, zrcv, load_s, hist_s, fwd_s, arr_s, relay_s, ext_s, x_r, ext_r, s0, r0, ms, mr, zs, zr,
    ready, near
):
    block_len, sensors, params = k_ref.shape
    fields = xbuf.shape[2]
    steps = out_ref.shape[0]
    piece = block_len // tm_count
    pieces = steps * tm_count
    last = pieces - 1
    half = piece // 2
    split = last - 1
    spans = [(c * piece, piece) for c in range(split)]
    spans += [(split * piece, half), (split * piece + half, piece - half), (last * piece, piece)]
    chunks = len(spans)
    rows = sensors // (tm_count * group * 2)
    share = sensors // (2 * group)
    k = lax.axis_index("tm")
    par = lax.axis_index("par")
    core, chip = par % 2, par // 2
    partner = par + 1 - 2 * core
    flips = sorted(range(1, group), key=lambda flip: -flip.bit_count())
    top = tm_count - 1

    def flipped(flip):
        target = chip
        for b in range(flip.bit_length()):
            if flip >> b & 1:
                target = target + (1 - 2 * ((chip // (1 << b)) % 2)) * (1 << b)
        return target

    order = [
        (tm * group + q) * 2 + half
        for half in range(2)
        for q in range(group)
        for tm in range(tm_count)
    ]

    def remote(src, dst, send, recv, where):
        return pltpu.make_async_remote_copy(
            src_ref=src, dst_ref=dst, send_sem=send, recv_sem=recv, device_id=where,
            device_id_type=MESH,
        )

    def signal(sem, where):
        pl.semaphore_signal(sem, inc=1, device_id=where, device_id_type=MESH)

    barrier = pltpu.get_barrier_semaphore()
    bits = [1 << b for b in range(group.bit_length() - 1)]
    pl.when(k > 0)(lambda: signal(barrier, {"tm": jnp.maximum(k - 1, 0)}))
    pl.when(k < top)(lambda: signal(barrier, {"tm": jnp.minimum(k + 1, top)}))
    for d in bits:
        signal(barrier, {"par": flipped(d) * 2 + core})
    signal(barrier, {"par": partner})

    history_load = pltpu.make_async_copy(h_ref, xbuf.at[pl.ds(0, block_len)], load_s.at[0])
    kernel_loads = [
        pltpu.make_async_copy(
            k_ref.at[block_len - 1 - j], kflat.at[:, pl.ds(j * params, params)], load_s.at[1]
        )
        for j in range(block_len)
    ]
    first_pieces = []
    for s in range(steps):
        place = xbuf.at[pl.ds(block_len * (s + 1), piece)]
        first_pieces.append(pltpu.make_async_copy(a_ref.at[s], place, load_s.at[2 + s]))
    place = xbuf.at[pl.ds(2 * block_len + piece, piece)]
    own_piece = pltpu.make_async_copy(a_ref.at[0], place, load_s.at[2])

    arrival_load = pltpu.make_async_copy(a_ref, abuf, load_s.at[2 + steps])

    history_load.start()
    arrival_load.start()
    for copy in kernel_loads:
        copy.start()

    @pl.when(k == 0)
    def _():
        for copy in first_pieces:
            copy.start()

    pl.when(k == 1)(own_piece.start)

    wide = 2 * piece
    @pl.when((k > 0) & (k < top - 1))
    def _():
        kext[:, pl.ds(0, piece * params)] = jnp.zeros((sensors, piece * params), BF16)

    @pl.when((k > 1) & (k < top))
    def _():
        tail = xbuf.at[pl.ds(block_len + last * piece, piece)]
        tail[...] = jnp.zeros(tail.shape, BF16)

    @pl.when(k == top)
    def _():
        xbuf[pl.ds(block_len + split * piece, 1)] = jnp.zeros((1, params, fields), BF16)

    zext[pl.ds(0, wide - 1 + piece)] = jnp.zeros((wide - 1 + piece, params, fields), BF16)

    around = (k < top).astype(jnp.int32) + (k > 0).astype(jnp.int32)
    pl.semaphore_wait(barrier, 1 + len(bits) + around)

    def slot(c):
        return xbuf.at[pl.ds(block_len + c * piece, piece)]

    up, down = {"tm": jnp.minimum(k + 1, top)}, {"tm": jnp.maximum(k - 1, 0)}
    sends_up = k < top
    forwards = (k > 0) & (k < top)

    history_copies = [
        remote(xbuf.at[pl.ds(i * piece, piece)], slot(i), hist_s, x_r.at[i], up)
        for i in range(tm_count)
    ]

    def parts(c):
        if c == split:
            return [(0, half, c), (half, piece - half, pieces)]
        return [(0, piece, c)]

    def into(c, src, send, where):
        return [
            remote(
                src.at[pl.ds(first, count)],
                xbuf.at[pl.ds(block_len + c * piece + first, count)],
                send, x_r.at[sem], where,
            )
            for first, count, sem in parts(c)
        ]

    forward_copies = [
        into(i + tm_count, slot(i), fwd_s, up) for i in range(tm_count - 1)
    ]

    def arrivals_from(step, s, target, c):
        copies = into(c, abuf.at[s], arr_s.at[s], {"tm": target})
        return [(k == step, copy) for copy in copies]

    near_copies = arrivals_from(0, 0, 1, tm_count)
    near_copies += arrivals_from(1, 0, 0, 1) + arrivals_from(1, 1, 0, tm_count + 1)
    near_copies += arrivals_from(2, 0, 1, tm_count + 2)
    far_copies, late_copies = [], []
    for i in range(2, tm_count):
        if i > 2:
            far_copies += arrivals_from(i, 0, (i + 1) % 2, i if i % 2 else tm_count + i)
        late_copies += arrivals_from(i, 1, 0, tm_count + i)
    evens, odds = range(2, tm_count, 2), range(3, tm_count, 2)
    relay_copies = {
        i: remote(slot(tm_count + i), slot(i), relay_s, x_r.at[i], {"tm": 0}) for i in evens
    } | {
        i: remote(slot(i), slot(tm_count + i), relay_s, x_r.at[tm_count + i], {"tm": 1})
        for i in odds
    }
    def ext_copy(n, begin=0, count=piece):
        first = (block_len - (n + 1) * piece + begin) * params
        source = kflat.at[:, pl.ds(first, count * params)]
        place = kext.at[:, pl.ds(((1 - n) * piece + begin) * params, count * params)]
        return remote(source, place, ext_s, ext_r.at[n], down)

    sends_ext = k > 1

    history_load.wait()

    @pl.when(sends_up)
    def _():
        for copy in history_copies:
            copy.start()

    arrival_load.wait()
    for condition, copy in near_copies:
        pl.when(condition)(copy.start)

    pltpu.make_async_copy(kflat, kflat, load_s.at[1]).wait()
    pl.when(k == top)(ext_copy(1, 0, 1).start)
    pl.when(k > 0)(lambda: pl.semaphore_wait(ready, 1))
    pl.when(sends_up)(lambda: signal(ready, up))

    for condition, copy in far_copies:
        pl.when(condition)(copy.start)

    if bits[1:]:
        signal(near.at[0], {"par": flipped(1) * 2 + core})

    pl.when(sends_ext)(ext_copy(0).start)
    pl.when(k == top)(ext_copy(1, 1, piece - 1).start)

    @pl.when(k == 0)
    def _():
        for copy in first_pieces:
            copy.wait()

    pl.when(k == 1)(own_piece.wait)

    for n, d in enumerate(bits[:-1]):
        pl.semaphore_wait(near.at[n], 1)
        if n + 1 < len(bits) - 1:
            signal(near.at[n + 1], {"par": flipped(bits[n + 1]) * 2 + core})

    def taken(unit):
        c = split if unit == pieces else unit
        first, count = [(f, n) for f, n, sem in parts(c) if sem == unit][0]
        place = xbuf.at[pl.ds(block_len + c * piece + first, count)]
        return remote(place, place, hist_s, x_r.at[unit], up)

    def receive(unit):
        c = split if unit == pieces else unit
        i = c % tm_count
        waits = k >= 0
        if i == c:
            waits = (k != 0) if c == 0 or c in odds else waits
        elif i < 2:
            waits = k != i
        elif i % 2 == 0:
            waits = k != 1
        if c == last:
            waits = waits & (k < 2)
        if c == split:
            waits = waits & (k < top)
        pl.when(waits)(taken(unit).wait_recv)

    def relay():
        @pl.when(k == 1)
        def _():
            for i in evens:
                for _, _, unit in parts(tm_count + i):
                    taken(unit).wait_recv()
                relay_copies[i].start()

        @pl.when(k == 0)
        def _():
            for i in odds:
                taken(i).wait_recv()
                relay_copies[i].start()

    def late():
        for condition, copy in late_copies:
            pl.when(condition)(copy.start)

    def span(c):
        return pl.ds(*spans[c])

    def flat_span(c):
        first, count = spans[c]
        return pl.ds(first * rows, count * rows)

    def core_copy(c):
        return remote(
            buf0.at[1 - core, :, span(c)], rcv0.at[:, span(c)], s0, r0.at[c],
            {"par": partner},
        )

    def chip_copy(c, d):
        target = flipped(d)
        return remote(
            mid.at[target, span(c)], mrcv.at[d - 1, span(c)], ms, mr.at[c],
            {"par": target * 2 + core},
        )

    def tm_copy(c, d):
        target = lax.rem(k + d, tm_count)
        place = flat_span(c)
        return remote(
            zbuf.at[target, place], zrcv.at[d - 1, place], zs, zr.at[tm_sem(c)],
            {"tm": target},
        )

    def tm_sem(c):
        return max(c - (split - 2), 0)

    def product(r, low, high):
        count = (high - low) * params
        left = xbuf[pl.ds(r + 1 + low, high - low)].reshape(count, fields)
        right = xbuf[pl.ds(r + 2 + low, high - low)].reshape(count, fields)
        both = jnp.concatenate([left, right], 1)
        lags = kflat[:, low * params : high * params]
        return jnp.dot(lags, both, preferred_element_type=F32)

    def hand_over(r, total):
        for side in range(2):
            mine = total[:, side * fields : (side + 1) * fields]
            moved = jnp.concatenate([mine[o * rows : (o + 1) * rows] for o in order], 0)
            moved = moved.astype(BF16)
            for n in range(2 * group):
                buf0[n // group, n % group, r + side] = moved[n * share : (n + 1) * share]

    def compute(c):
        receive(c)
        if c < tm_count - 1:

            @pl.when(forwards & (k < top - 1) if c == tm_count - 2 else forwards)
            def _():
                for copy in forward_copies[c]:
                    copy.start()

        first, count = spans[c]
        for r in range(first, first + count, 2):
            hand_over(r, product(r, 0, block_len))
        core_copy(c).start()

    begin = (split - 1) * piece
    last_rows = list(enumerate(range(begin, steps * block_len, 2)))
    latest = [(n, r) for n, r in last_rows if r >= split * piece]

    def bound(r, c):
        return block_len + c * piece - r - 2

    def early():
        for n, r in last_rows:
            acc[n] = product(r, 0, bound(r, split - 1))

    def extra():
        rest = 2 * block_len - wide
        zext[pl.ds(wide - 1 + piece, piece)] = xbuf[pl.ds(rest + piece, piece)]

        @pl.when(k == top - 1)
        def _():
            zext[pl.ds(wide - 1, piece)] = xbuf[pl.ds(rest, piece)]
            ext_copy(1).wait_recv()

        ext_copy(0).wait_recv()
        left = zext[pl.ds(wide - 2, wide)].reshape(wide * params, fields)
        right = zext[pl.ds(wide - 1, wide)].reshape(wide * params, fields)
        both = jnp.concatenate([left, right], 1)
        for n, r in latest:
            count = (r + 2 - split * piece) * params
            lags = kext[:, wide * params - count :]
            acc[n] = acc[n] + jnp.dot(lags, both[:count], preferred_element_type=F32)

    def middle():
        for n, r in latest:
            acc[n] = acc[n] + product(r, bound(r, split - 1), bound(r, split))

    def final(c):
        receive((split - 1, split, pieces, last)[c - split + 1])
        first, count = spans[c]
        for r in range(first, first + count, 2):
            n = (r - begin) // 2
            hand_over(r, acc[n] + product(r, bound(r, min(c, split)), block_len))
        core_copy(c).start()

    def close(c):
        first, count = spans[c]
        for r in range(first, first + count, 2):
            n = (r - begin) // 2
            hand_over(r, acc[n] + product(r, bound(r, split - 1), bound(r, split) + 1))
        core_copy(c).start()

    def across(c):
        core_copy(c).wait_recv()
        total = buf0[core, :, span(c)].astype(F32) + rcv0[:, span(c)].astype(F32)
        mid[:, span(c)] = total.astype(BF16)
        for d in flips:
            chip_copy(c, d).start()

    def goes_up(d):
        return k + d < tm_count

    def spread(c):
        total = mid[chip, span(c)].astype(F32)
        place = mrcv.at[:, span(c)]
        remote(place, place, ms, mr.at[c], {"par": par}).wait_recv()
        for d in range(1, group):
            total = total + mrcv[d - 1, span(c)].astype(F32)
        for t in range(tm_count):
            mine = [total[g, t * rows : (t + 1) * rows] for g in range(spans[c][1])]
            zbuf[t, flat_span(c)] = jnp.concatenate(mine, 0).astype(BF16)
        for d in range(1, tm_count):
            pl.when(jnp.logical_not(goes_up(d)))(tm_copy(c, d).start)

    def rise(c):
        for d in range(1, tm_count):
            pl.when(goes_up(d))(tm_copy(c, d).start)

    def finish(c):
        place = flat_span(c)
        total = zbuf[k, place].astype(F32)
        if tm_sem(c):
            taken_parts = zrcv.at[:, place]
        else:
            taken_parts = zrcv.at[:, pl.ds(0, (split - 1) * piece * rows)]
        if tm_sem(c) or c == 0:
            remote(taken_parts, taken_parts, zs, zr.at[tm_sem(c)], {"tm": k}).wait_recv()
        for d in range(1, tm_count):
            total = total + zrcv[d - 1, place].astype(F32)
        first, count = spans[c]
        total = total.reshape(count, rows, fields).astype(out_ref.dtype)
        first = first % block_len
        out_ref[spans[c][0] // block_len, first : first + count] = total

    def across_on(which, c):
        pl.when(core == which)(lambda: across(c))

    def run(plan):
        for stage, *c in plan:
            stage(*c)

    ends = [(across, split + 1), (across, split + 2), (spread, split - 2)]
    ends += [(rise, c) for c in range(split - 1)]
    ends += [(spread, split - 1), (rise, split - 1)]
    for c in range(split, chunks):
        ends += [(spread, c), (rise, c)]

    @pl.when(k == 0)
    def _():
        plan = [(compute, 0), (across, 0), (compute, 1), (relay,), (across, 1), (spread, 0)]
        for c in range(2, split - 1):
            plan.append((compute, c))
            if c > 2:
                plan.append((across, c - 1))
            if c > 3:
                plan.append((spread, c - 3))
        plan += [(early,), (final, split - 1), (across, split - 2), (spread, split - 4)]
        plan += [(across, split - 1), (spread, split - 3), (middle,)]
        plan += [(final, c) for c in range(split, chunks)]
        run(plan + [(across, split)] + ends)

    def paced(tail):
        plan = []
        for c in range(split - 1):
            plan.append((compute, c))
            if c == split - 2:
                plan += [(across_on, 0, c), (early,)]
            else:
                plan.append((across, c))
            if c == 0:
                plan.append((relay,))
            if c == 2:
                plan.append((late,))
            if 2 <= c < split - 2:
                plan.append((spread, c - 2))
        run(plan + [(spread, split - 4)] + tail + ends)

    @pl.when(forwards)
    def _():
        tail = [(extra,), (final, split - 1), (across_on, 1, split - 2)]
        tail += [(across_on, 0, split - 1), (middle,), (final, split), (across_on, 0, split)]
        tail += [(final, split + 1), (final, split + 2), (across_on, 1, split - 1)]
        paced(tail + [(across_on, 1, split), (spread, split - 3)])

    @pl.when(k == top)
    def _():
        tail = [(final, split - 1), (across_on, 0, split - 1), (close, split)]
        tail += [(across_on, 0, split), (across_on, 1, split - 2), (close, split + 1)]
        tail += [(close, split + 2), (across_on, 1, split - 1), (across_on, 1, split)]
        paced(tail + [(spread, split - 3)])

    run([(finish, c) for c in range(chunks)])

    def sent(place, sem):
        return remote(place, place, sem, x_r.at[0], up).wait_send

    pl.when(sends_up)(sent(xbuf.at[pl.ds(0, block_len)], hist_s))
    pl.when(forwards)(sent(xbuf.at[pl.ds(0, block_len - wide)], fwd_s))
    pl.when(forwards & (k < top - 1))(sent(xbuf.at[pl.ds(0, piece)], fwd_s))
    sent(abuf.at[0], arr_s.at[0])()
    pl.when(k > 0)(sent(abuf.at[1], arr_s.at[1]))
    for step, those in ((1, evens), (0, odds)):
        if those:
            pl.when(k == step)(sent(xbuf.at[pl.ds(0, len(those) * piece)], relay_s))
    pl.when(sends_ext)(ext_copy(0).wait_send)
    pl.when(k == top)(ext_copy(1).wait_send)
    sent(rcv0, s0)()
    sent(mrcv, ms)()
    sent(zrcv, zs)()


def fused(tm_count, group, kernel, history, arrivals):
    block_len, sensors, params = kernel.shape
    fields = history.shape[2]
    steps = arrivals.shape[0]
    piece = block_len // tm_count
    pieces = steps * tm_count
    outputs = steps * block_len
    share = sensors // (2 * group)
    rows = share // tm_count
    dma = pltpu.SemaphoreType.DMA
    scratch = [
        pltpu.VMEM((sensors, block_len * params), BF16),
        pltpu.VMEM((sensors, 2 * piece * params), BF16),
        pltpu.VMEM(((steps + 1) * block_len, params, fields), BF16),
        pltpu.VMEM((steps, piece, params, fields), BF16),
        pltpu.VMEM((4 * piece - 1, params, fields), BF16),
        pltpu.VMEM((piece + piece // 2, sensors, 2 * fields), F32),
        pltpu.VMEM((2, group, outputs, share, fields), BF16),
        pltpu.VMEM((group, outputs, share, fields), BF16),
        pltpu.VMEM((group, outputs, share, fields), BF16),
        pltpu.VMEM((group - 1, outputs, share, fields), BF16),
        pltpu.VMEM((tm_count, outputs * rows, fields), BF16),
        pltpu.VMEM((tm_count - 1, outputs * rows, fields), BF16),
        dma((3 + steps,)),
        dma(()),
        dma(()),
        dma((2,)),
        dma(()),
        dma(()),
        dma((pieces + 1,)),
        dma((2,)),
        dma(()),
        dma((pieces + 1,)),
        dma(()),
        dma((pieces + 1,)),
        dma(()),
        dma((5,)),
        pltpu.SemaphoreType.REGULAR,
        pltpu.SemaphoreType.REGULAR((max(group.bit_length() - 2, 1),)),
    ]
    out_bytes = steps * block_len * rows * fields * 2
    return pl.pallas_call(
        functools.partial(kernel_body, tm_count, group),
        out_shape=pltpu.VMEM((steps, block_len, rows, fields), BF16),
        in_specs=[pl.BlockSpec(memory_space=pltpu.HBM)] * 3,
        out_specs=pl.BlockSpec(memory_space=pltpu.VMEM),
        scratch_shapes=scratch,
        compiler_params=pltpu.CompilerParams(
            collective_id=0, has_side_effects=True, vmem_limit_bytes=VMEM_BYTES - 2 * out_bytes
        ),
    )(kernel, history, arrivals)


def plain(tm_count, kernel, history, arrivals):
    block_len, sensors, params = kernel.shape
    fields = history.shape[2]
    steps = arrivals.shape[0]
    incoming = lax.all_gather(arrivals, "tm", axis=1, tiled=True)
    position = lax.axis_index("tm")
    pairs = [(i, i + 1) for i in range(tm_count - 1)]
    blocks = [history]
    for s in range(steps):
        shifted = lax.ppermute(blocks[-1], "tm", pairs)
        blocks.append(jnp.where(position == 0, incoming[s], shifted))
    window = jnp.concatenate(blocks, 0)
    flat = kernel[::-1].transpose(1, 0, 2).reshape(sensors, block_len * params)

    def one(first):
        part = lax.dynamic_slice_in_dim(window, first, block_len, 0)
        part = part.reshape(block_len * params, fields)
        return jnp.dot(flat, part, preferred_element_type=F32)

    partial = lax.map(one, jnp.arange(steps * block_len, dtype=jnp.int32) + 1)
    partial = partial.reshape(steps, block_len, sensors, fields)
    total = lax.psum_scatter(partial, ("tm", "par"), scatter_dimension=2, tiled=True)
    return total.astype(BF16)


def solution(mesh):
    tm_count, par_count = mesh.shape["tm"], mesh.shape["par"]

    def per_device(kernel, history, arrivals):
        rows = kernel.shape[1] // (tm_count * par_count)
        piece = kernel.shape[0] // tm_count
        fits = rows % 8 == 0 and piece % 4 == 0 and tm_count > 3 and arrivals.shape[0] == 2
        if fits and par_count > 2 and par_count.bit_count() == 1:
            return fused(tm_count, par_count // 2, kernel, history, arrivals)
        return plain(tm_count, kernel, history, arrivals)

    in_specs = (P("tm", None, "par"), P("tm", "par", None), P(None, "tm", "par", None))
    out_specs = P(None, None, ("tm", "par"), None)
    return jax.shard_map(
        per_device, mesh=mesh, in_specs=in_specs, out_specs=out_specs, check_vma=False
    )
```

```python
import functools

import jax
import jax.numpy as jnp
from jax import lax
from jax.experimental import pallas as pl
from jax.experimental.pallas import tpu as pltpu
from jax.sharding import PartitionSpec as P

MESH = pl.DeviceIdType.MESH
F32 = jnp.float32
BF16 = jnp.bfloat16
VMEM_BYTES = 67_043_328
LATE = 2


def kernel_body(
    tm_count, group, k_ref, h_ref, a_ref, out_ref, kflat, kext, xbuf, abuf, zext, acc, buf0, rcv0, mid, mrcv,
    zbuf, zrcv, load_s, hist_s, fwd_s, arr_s, relay_s, ext_s, x_r, ext_r, s0, r0, ms, mr, zs, zr,
    ready, near
):
    block_len, sensors, params = k_ref.shape
    fields = xbuf.shape[2]
    steps = out_ref.shape[0]
    piece = block_len // tm_count
    pieces = steps * tm_count
    last = pieces - 1
    half = piece // 2
    split = last - 1
    spans = [(c * piece, piece) for c in range(split)]
    spans += [(split * piece, half), (split * piece + half, piece - half), (last * piece, piece)]
    chunks = len(spans)
    rows = sensors // (tm_count * group * 2)
    share = sensors // (2 * group)
    k = lax.axis_index("tm")
    par = lax.axis_index("par")
    core, chip = par % 2, par // 2
    partner = par + 1 - 2 * core
    flips = sorted(range(1, group), key=lambda flip: -flip.bit_count())
    top = tm_count - 1

    def flipped(flip):
        target = chip
        for b in range(flip.bit_length()):
            if flip >> b & 1:
                target = target + (1 - 2 * ((chip // (1 << b)) % 2)) * (1 << b)
        return target

    order = [
        (tm * group + q) * 2 + half
        for half in range(2)
        for q in range(group)
        for tm in range(tm_count)
    ]

    def remote(src, dst, send, recv, where):
        return pltpu.make_async_remote_copy(
            src_ref=src, dst_ref=dst, send_sem=send, recv_sem=recv, device_id=where,
            device_id_type=MESH,
        )

    def signal(sem, where):
        pl.semaphore_signal(sem, inc=1, device_id=where, device_id_type=MESH)

    barrier = pltpu.get_barrier_semaphore()
    bits = [1 << b for b in range(group.bit_length() - 1)]
    pl.when(k > 0)(lambda: signal(barrier, {"tm": jnp.maximum(k - 1, 0)}))
    pl.when(k < top)(lambda: signal(barrier, {"tm": jnp.minimum(k + 1, top)}))
    for d in bits:
        signal(barrier, {"par": flipped(d) * 2 + core})
    signal(barrier, {"par": partner})

    history_load = pltpu.make_async_copy(h_ref, xbuf.at[pl.ds(0, block_len)], load_s.at[0])
    kernel_loads = [
        pltpu.make_async_copy(
            k_ref.at[block_len - 1 - j], kflat.at[:, pl.ds(j * params, params)], load_s.at[1]
        )
        for j in range(block_len)
    ]
    first_pieces = []
    for s in range(steps):
        place = xbuf.at[pl.ds(block_len * (s + 1), piece)]
        first_pieces.append(pltpu.make_async_copy(a_ref.at[s], place, load_s.at[2 + s]))
    place = xbuf.at[pl.ds(2 * block_len + piece, piece)]
    own_piece = pltpu.make_async_copy(a_ref.at[0], place, load_s.at[2])

    arrival_load = pltpu.make_async_copy(a_ref, abuf, load_s.at[2 + steps])

    history_load.start()
    arrival_load.start()
    for copy in kernel_loads:
        copy.start()

    @pl.when(k == 0)
    def _():
        for copy in first_pieces:
            copy.start()

    pl.when(k == 1)(own_piece.start)

    wide = 2 * piece
    @pl.when((k > 0) & (k < top - 1))
    def _():
        kext[:, pl.ds(0, half * params)] = jnp.zeros((sensors, half * params), BF16)

    @pl.when((k > 0) & (k < top - 1) & (core == 1))
    def _():
        rest = (piece - half) * params
        kext[:, pl.ds(half * params, rest)] = jnp.zeros((sensors, rest), BF16)

    @pl.when((k > 1) & (k < top))
    def _():
        tail = xbuf.at[pl.ds(block_len + last * piece, piece)]
        tail[...] = jnp.zeros(tail.shape, BF16)

    @pl.when((k > 1) & (k < top) & (core == 0))
    def _():
        tail = xbuf.at[pl.ds(block_len + split * piece + half, piece - half)]
        tail[...] = jnp.zeros(tail.shape, BF16)

    @pl.when(k == top)
    def _():
        xbuf[pl.ds(block_len + split * piece, 1)] = jnp.zeros((1, params, fields), BF16)

    zext[pl.ds(0, wide - 1 + piece)] = jnp.zeros((wide - 1 + piece, params, fields), BF16)

    around = (k < top).astype(jnp.int32) + (k > 0).astype(jnp.int32)
    pl.semaphore_wait(barrier, 1 + len(bits) + around)

    def slot(c):
        return xbuf.at[pl.ds(block_len + c * piece, piece)]

    up, down = {"tm": jnp.minimum(k + 1, top)}, {"tm": jnp.maximum(k - 1, 0)}
    sends_up = k < top
    forwards = (k > 0) & (k < top)

    history_copies = [
        remote(xbuf.at[pl.ds(i * piece, piece)], slot(i), hist_s, x_r.at[i], up)
        for i in range(tm_count)
    ]

    def parts(c):
        if c == split:
            return [(0, half, c), (half, piece - half, pieces)]
        return [(0, piece, c)]

    def into(c, src, send, where):
        return [
            remote(
                src.at[pl.ds(first, count)],
                xbuf.at[pl.ds(block_len + c * piece + first, count)],
                send, x_r.at[sem], where,
            )
            for first, count, sem in parts(c)
        ]

    forward_copies = [
        into(i + tm_count, slot(i), fwd_s, up) for i in range(tm_count - 1)
    ]

    def arrivals_from(step, s, target, c):
        copies = into(c, abuf.at[s], arr_s.at[s], {"tm": target})
        return [(k == step, copy) for copy in copies]

    near_copies = arrivals_from(0, 0, 1, tm_count)
    near_copies += arrivals_from(1, 0, 0, 1) + arrivals_from(1, 1, 0, tm_count + 1)
    near_copies += arrivals_from(2, 0, 1, tm_count + 2)
    far_copies, late_copies = [], []
    for i in range(2, tm_count):
        if i > 2:
            far_copies += arrivals_from(i, 0, (i + 1) % 2, i if i % 2 else tm_count + i)
        late_copies += arrivals_from(i, 1, 0, tm_count + i)
    evens, odds = range(2, tm_count, 2), range(3, tm_count, 2)
    relay_copies = {
        i: remote(slot(tm_count + i), slot(i), relay_s, x_r.at[i], {"tm": 0}) for i in evens
    } | {
        i: remote(slot(i), slot(tm_count + i), relay_s, x_r.at[tm_count + i], {"tm": 1})
        for i in odds
    }
    def ext_copy(n, begin=0, count=piece):
        first = (block_len - (n + 1) * piece + begin) * params
        source = kflat.at[:, pl.ds(first, count * params)]
        place = kext.at[:, pl.ds(((1 - n) * piece + begin) * params, count * params)]
        return remote(source, place, ext_s, ext_r.at[n], down)

    sends_ext = k > 1

    history_load.wait()

    @pl.when(sends_up)
    def _():
        for copy in history_copies:
            copy.start()

    arrival_load.wait()
    for condition, copy in near_copies:
        pl.when(condition)(copy.start)

    pltpu.make_async_copy(kflat, kflat, load_s.at[1]).wait()
    pl.when(k == top)(ext_copy(1, 0, 1).start)
    pl.when(k > 0)(lambda: pl.semaphore_wait(ready, 1))
    pl.when(sends_up)(lambda: signal(ready, up))

    for condition, copy in far_copies:
        pl.when(condition)(copy.start)

    if bits[1:]:
        signal(near.at[0], {"par": flipped(1) * 2 + core})

    pl.when(sends_ext)(ext_copy(0).start)
    pl.when(k == top)(ext_copy(1, 1, piece - 1).start)
    more = (k > 1) & (k < top) & (core == 0)
    pl.when(more)(ext_copy(1, half, piece - half).start)

    @pl.when(k == 0)
    def _():
        for copy in first_pieces:
            copy.wait()

    pl.when(k == 1)(own_piece.wait)

    for n, d in enumerate(bits[:-1]):
        pl.semaphore_wait(near.at[n], 1)
        if n + 1 < len(bits) - 1:
            signal(near.at[n + 1], {"par": flipped(bits[n + 1]) * 2 + core})

    def taken(unit):
        c = split if unit == pieces else unit
        first, count = [(f, n) for f, n, sem in parts(c) if sem == unit][0]
        place = xbuf.at[pl.ds(block_len + c * piece + first, count)]
        return remote(place, place, hist_s, x_r.at[unit], up)

    def receive(unit):
        c = split if unit == pieces else unit
        i = c % tm_count
        waits = k >= 0
        if i == c:
            waits = (k != 0) if c == 0 or c in odds else waits
        elif i < 2:
            waits = k != i
        elif i % 2 == 0:
            waits = k != 1
        if c == last:
            waits = waits & (k < 2)
        if unit == pieces:
            waits = waits & ((k < 2) | ((k < top) & (core == 1)))
        elif c == split:
            waits = waits & (k < top)
        pl.when(waits)(taken(unit).wait_recv)

    def relay():
        @pl.when(k == 1)
        def _():
            for i in evens:
                for _, _, unit in parts(tm_count + i):
                    taken(unit).wait_recv()
                relay_copies[i].start()

        @pl.when(k == 0)
        def _():
            for i in odds:
                taken(i).wait_recv()
                relay_copies[i].start()

    def late():
        for condition, copy in late_copies:
            pl.when(condition)(copy.start)

    def span(c):
        return pl.ds(*spans[c])

    def flat_span(c):
        first, count = spans[c]
        return pl.ds(first * rows, count * rows)

    def core_copy(c):
        return remote(
            buf0.at[1 - core, :, span(c)], rcv0.at[:, span(c)], s0, r0.at[c],
            {"par": partner},
        )

    def chip_copy(c, d):
        target = flipped(d)
        return remote(
            mid.at[target, span(c)], mrcv.at[d - 1, span(c)], ms, mr.at[c],
            {"par": target * 2 + core},
        )

    def tm_copy(c, d):
        target = lax.rem(k + d, tm_count)
        place = flat_span(c)
        return remote(
            zbuf.at[target, place], zrcv.at[d - 1, place], zs, zr.at[tm_sem(c)],
            {"tm": target},
        )

    def tm_sem(c):
        return max(c - (split - 2), 0)

    def product(r, low, high):
        count = (high - low) * params
        left = xbuf[pl.ds(r + 1 + low, high - low)].reshape(count, fields)
        right = xbuf[pl.ds(r + 2 + low, high - low)].reshape(count, fields)
        both = jnp.concatenate([left, right], 1)
        lags = kflat[:, low * params : high * params]
        return jnp.dot(lags, both, preferred_element_type=F32)

    def hand_over(r, total):
        for side in range(2):
            mine = total[:, side * fields : (side + 1) * fields]
            moved = jnp.concatenate([mine[o * rows : (o + 1) * rows] for o in order], 0)
            moved = moved.astype(BF16)
            for n in range(2 * group):
                buf0[n // group, n % group, r + side] = moved[n * share : (n + 1) * share]

    def compute(c):
        receive(c)
        if c < tm_count - 1:

            goes = forwards & (k < top - 1) if c == tm_count - 2 else forwards
            pl.when(goes)(forward_copies[c][0].start)
            for copy in forward_copies[c][1:]:
                pl.when(goes & (core == 1))(copy.start)

        first, count = spans[c]
        for r in range(first, first + count, 2):
            hand_over(r, product(r, 0, block_len))
        core_copy(c).start()

    begin = (split - 1) * piece
    last_rows = list(enumerate(range(begin, steps * block_len, 2)))
    latest = [(n, r) for n, r in last_rows if r >= split * piece]

    def bound(r, c):
        return block_len + c * piece - r - 2

    def early():
        for n, r in last_rows:
            acc[n] = product(r, 0, bound(r, split - 1))

    def extra():
        rest = 2 * block_len - wide
        zext[pl.ds(wide - 1 + piece, piece)] = xbuf[pl.ds(rest + piece, piece)]

        @pl.when(k == top - 1)
        def _():
            zext[pl.ds(wide - 1, piece)] = xbuf[pl.ds(rest, piece)]
            ext_copy(1).wait_recv()

        @pl.when((k < top - 1) & (core == 0))
        def _():
            zext[pl.ds(wide - 1 + half, piece - half)] = xbuf[pl.ds(rest + half, piece - half)]
            ext_copy(1, half, piece - half).wait_recv()

        ext_copy(0).wait_recv()
        left = zext[pl.ds(wide - 2, wide)].reshape(wide * params, fields)
        right = zext[pl.ds(wide - 1, wide)].reshape(wide * params, fields)
        both = jnp.concatenate([left, right], 1)
        for n, r in latest:
            count = (r + 2 - split * piece) * params
            lags = kext[:, wide * params - count :]
            acc[n] = acc[n] + jnp.dot(lags, both[:count], preferred_element_type=F32)

    def middle():
        for n, r in latest:
            acc[n] = acc[n] + product(r, bound(r, split - 1), bound(r, split))

    def final(c):
        receive((split - 1, split, pieces, last)[c - split + 1])
        first, count = spans[c]
        for r in range(first, first + count, 2):
            n = (r - begin) // 2
            hand_over(r, acc[n] + product(r, bound(r, min(c, split)), block_len))
        core_copy(c).start()

    def close(c):
        first, count = spans[c]
        for r in range(first, first + count, 2):
            n = (r - begin) // 2
            hand_over(r, acc[n] + product(r, bound(r, split - 1), bound(r, split) + 1))
        core_copy(c).start()

    def across(c):
        core_copy(c).wait_recv()
        total = buf0[core, :, span(c)].astype(F32) + rcv0[:, span(c)].astype(F32)
        mid[:, span(c)] = total.astype(BF16)
        for d in flips:
            chip_copy(c, d).start()

    def goes_up(d):
        return k + d < tm_count

    def spread(c):
        total = mid[chip, span(c)].astype(F32)
        place = mrcv.at[:, span(c)]
        remote(place, place, ms, mr.at[c], {"par": par}).wait_recv()
        for d in range(1, group):
            total = total + mrcv[d - 1, span(c)].astype(F32)
        for t in range(tm_count):
            mine = [total[g, t * rows : (t + 1) * rows] for g in range(spans[c][1])]
            zbuf[t, flat_span(c)] = jnp.concatenate(mine, 0).astype(BF16)
        for d in range(1, tm_count):
            pl.when(jnp.logical_not(goes_up(d)))(tm_copy(c, d).start)

    def rise(c):
        for d in range(1, tm_count):
            pl.when(goes_up(d))(tm_copy(c, d).start)

    def finish(c):
        place = flat_span(c)
        total = zbuf[k, place].astype(F32)
        if tm_sem(c):
            taken_parts = zrcv.at[:, place]
        else:
            taken_parts = zrcv.at[:, pl.ds(0, (split - 1) * piece * rows)]
        if tm_sem(c) or c == 0:
            remote(taken_parts, taken_parts, zs, zr.at[tm_sem(c)], {"tm": k}).wait_recv()
        for d in range(1, tm_count):
            total = total + zrcv[d - 1, place].astype(F32)
        first, count = spans[c]
        total = total.reshape(count, rows, fields).astype(out_ref.dtype)
        first = first % block_len
        out_ref[spans[c][0] // block_len, first : first + count] = total

    def across_on(which, c):
        pl.when(core == which)(lambda: across(c))

    def run(plan):
        for stage, *c in plan:
            stage(*c)

    ends = [(across, split + 1), (across, split + 2), (spread, split - 2)]
    ends += [(rise, c) for c in range(split - 1)]
    ends += [(spread, split - 1), (rise, split - 1)]
    for c in range(split, chunks):
        ends += [(spread, c), (rise, c)]

    @pl.when(k == 0)
    def _():
        plan = [(compute, 0), (across, 0), (compute, 1), (relay,), (across, 1), (spread, 0)]
        for c in range(2, split - 1):
            plan.append((compute, c))
            if c > 2:
                plan.append((across, c - 1))
            if c > 3:
                plan.append((spread, c - 3))
        plan += [(early,), (final, split - 1), (across, split - 2), (spread, split - 4)]
        plan += [(across, split - 1), (spread, split - 3), (middle,)]
        plan += [(final, c) for c in range(split, chunks)]
        run(plan + [(across, split)] + ends)

    def paced(tail):
        plan = []
        for c in range(split - 1):
            plan.append((compute, c))
            if c == split - 2:
                plan += [(across_on, 0, c), (early,)]
            else:
                plan.append((across, c))
            if c == 0:
                plan.append((relay,))
            if c == 2:
                plan.append((late,))
            if 2 <= c < split - 2:
                plan.append((spread, c - 2))
        run(plan + [(spread, split - 4)] + tail + ends)

    @pl.when(forwards)
    def _():
        tail = [(extra,), (final, split - 1), (across_on, 1, split - 2)]
        tail += [(across_on, 0, split - 1), (middle,), (final, split), (across_on, 0, split)]
        tail += [(final, split + 1), (final, split + 2), (across_on, 1, split - 1)]
        paced(tail + [(across_on, 1, split), (spread, split - 3)])

    @pl.when(k == top)
    def _():
        tail = [(final, split - 1), (across_on, 0, split - 1), (close, split)]
        tail += [(across_on, 0, split), (across_on, 1, split - 2), (close, split + 1)]
        tail += [(close, split + 2), (across_on, 1, split - 1), (across_on, 1, split)]
        paced(tail + [(spread, split - 3)])

    run([(finish, c) for c in range(chunks)])

    def sent(place, sem):
        return remote(place, place, sem, x_r.at[0], up).wait_send

    pl.when(sends_up)(sent(xbuf.at[pl.ds(0, block_len)], hist_s))
    pl.when(forwards)(sent(xbuf.at[pl.ds(0, block_len - wide)], fwd_s))
    goes = forwards & (k < top - 1)
    pl.when(goes & (core == 0))(sent(xbuf.at[pl.ds(0, half)], fwd_s))
    pl.when(goes & (core == 1))(sent(xbuf.at[pl.ds(0, piece)], fwd_s))
    sent(abuf.at[0], arr_s.at[0])()
    pl.when(k > 0)(sent(abuf.at[1], arr_s.at[1]))
    for step, those in ((1, evens), (0, odds)):
        if those:
            pl.when(k == step)(sent(xbuf.at[pl.ds(0, len(those) * piece)], relay_s))
    pl.when(sends_ext)(ext_copy(0).wait_send)
    pl.when(k == top)(ext_copy(1).wait_send)
    pl.when(more)(ext_copy(1, half, piece - half).wait_send)
    sent(rcv0, s0)()
    sent(mrcv, ms)()
    sent(zrcv, zs)()


def fused(tm_count, group, kernel, history, arrivals):
    block_len, sensors, params = kernel.shape
    fields = history.shape[2]
    steps = arrivals.shape[0]
    piece = block_len // tm_count
    pieces = steps * tm_count
    outputs = steps * block_len
    share = sensors // (2 * group)
    rows = share // tm_count
    dma = pltpu.SemaphoreType.DMA
    scratch = [
        pltpu.VMEM((sensors, block_len * params), BF16),
        pltpu.VMEM((sensors, 2 * piece * params), BF16),
        pltpu.VMEM(((steps + 1) * block_len, params, fields), BF16),
        pltpu.VMEM((steps, piece, params, fields), BF16),
        pltpu.VMEM((4 * piece - 1, params, fields), BF16),
        pltpu.VMEM((piece + piece // 2, sensors, 2 * fields), F32),
        pltpu.VMEM((2, group, outputs, share, fields), BF16),
        pltpu.VMEM((group, outputs, share, fields), BF16),
        pltpu.VMEM((group, outputs, share, fields), BF16),
        pltpu.VMEM((group - 1, outputs, share, fields), BF16),
        pltpu.VMEM((tm_count, outputs * rows, fields), BF16),
        pltpu.VMEM((tm_count - 1, outputs * rows, fields), BF16),
        dma((3 + steps,)),
        dma(()),
        dma(()),
        dma((2,)),
        dma(()),
        dma(()),
        dma((pieces + 1,)),
        dma((2,)),
        dma(()),
        dma((pieces + 1,)),
        dma(()),
        dma((pieces + 1,)),
        dma(()),
        dma((5,)),
        pltpu.SemaphoreType.REGULAR,
        pltpu.SemaphoreType.REGULAR((max(group.bit_length() - 2, 1),)),
    ]
    out_bytes = steps * block_len * rows * fields * 2
    return pl.pallas_call(
        functools.partial(kernel_body, tm_count, group),
        out_shape=pltpu.VMEM((steps, block_len, rows, fields), BF16),
        in_specs=[pl.BlockSpec(memory_space=pltpu.HBM)] * 3,
        out_specs=pl.BlockSpec(memory_space=pltpu.VMEM),
        scratch_shapes=scratch,
        compiler_params=pltpu.CompilerParams(
            collective_id=0, has_side_effects=True, vmem_limit_bytes=VMEM_BYTES - 2 * out_bytes
        ),
    )(kernel, history, arrivals)


def plain(tm_count, kernel, history, arrivals):
    block_len, sensors, params = kernel.shape
    fields = history.shape[2]
    steps = arrivals.shape[0]
    incoming = lax.all_gather(arrivals, "tm", axis=1, tiled=True)
    position = lax.axis_index("tm")
    pairs = [(i, i + 1) for i in range(tm_count - 1)]
    blocks = [history]
    for s in range(steps):
        shifted = lax.ppermute(blocks[-1], "tm", pairs)
        blocks.append(jnp.where(position == 0, incoming[s], shifted))
    window = jnp.concatenate(blocks, 0)
    flat = kernel[::-1].transpose(1, 0, 2).reshape(sensors, block_len * params)

    def one(first):
        part = lax.dynamic_slice_in_dim(window, first, block_len, 0)
        part = part.reshape(block_len * params, fields)
        return jnp.dot(flat, part, preferred_element_type=F32)

    partial = lax.map(one, jnp.arange(steps * block_len, dtype=jnp.int32) + 1)
    partial = partial.reshape(steps, block_len, sensors, fields)
    total = lax.psum_scatter(partial, ("tm", "par"), scatter_dimension=2, tiled=True)
    return total.astype(BF16)


def solution(mesh):
    tm_count, par_count = mesh.shape["tm"], mesh.shape["par"]

    def per_device(kernel, history, arrivals):
        rows = kernel.shape[1] // (tm_count * par_count)
        piece = kernel.shape[0] // tm_count
        fits = rows % 8 == 0 and piece % 4 == 0 and tm_count > 3 and arrivals.shape[0] == 2
        if fits and par_count > 2 and par_count.bit_count() == 1:
            return fused(tm_count, par_count // 2, kernel, history, arrivals)
        return plain(tm_count, kernel, history, arrivals)

    in_specs = (P("tm", None, "par"), P("tm", "par", None), P(None, "tm", "par", None))
    out_specs = P(None, None, ("tm", "par"), None)
    return jax.shard_map(
        per_device, mesh=mesh, in_specs=in_specs, out_specs=out_specs, check_vma=False
    )
```

```python
import functools

import jax
import jax.numpy as jnp
from jax import lax
from jax.experimental import pallas as pl
from jax.experimental.pallas import tpu as pltpu
from jax.sharding import PartitionSpec as P

MESH = pl.DeviceIdType.MESH
F32 = jnp.float32
BF16 = jnp.bfloat16
VMEM_BYTES = 67_043_328
LATE = 2


def kernel_body(
    tm_count, group, k_ref, h_ref, a_ref, out_ref, kflat, kext, xbuf, abuf, zext, acc, buf0, rcv0, mid, mrcv,
    zbuf, zrcv, load_s, hist_s, fwd_s, arr_s, relay_s, ext_s, x_r, ext_r, s0, r0, ms, mr, zs, zr,
    ready, near
):
    block_len, sensors, params = k_ref.shape
    fields = xbuf.shape[2]
    steps = out_ref.shape[0]
    piece = block_len // tm_count
    pieces = steps * tm_count
    last = pieces - 1
    half = piece // 2
    split = last - 1
    spans = [(c * piece, piece) for c in range(split)]
    spans += [(split * piece, half), (split * piece + half, piece - half), (last * piece, piece)]
    chunks = len(spans)
    rows = sensors // (tm_count * group * 2)
    share = sensors // (2 * group)
    k = lax.axis_index("tm")
    par = lax.axis_index("par")
    core, chip = par % 2, par // 2
    partner = par + 1 - 2 * core
    flips = sorted(range(1, group), key=lambda flip: -flip.bit_count())
    top = tm_count - 1

    def flipped(flip):
        target = chip
        for b in range(flip.bit_length()):
            if flip >> b & 1:
                target = target + (1 - 2 * ((chip // (1 << b)) % 2)) * (1 << b)
        return target

    order = [
        (tm * group + q) * 2 + half
        for half in range(2)
        for q in range(group)
        for tm in range(tm_count)
    ]

    def remote(src, dst, send, recv, where):
        return pltpu.make_async_remote_copy(
            src_ref=src, dst_ref=dst, send_sem=send, recv_sem=recv, device_id=where,
            device_id_type=MESH,
        )

    def signal(sem, where):
        pl.semaphore_signal(sem, inc=1, device_id=where, device_id_type=MESH)

    barrier = pltpu.get_barrier_semaphore()
    bits = [1 << b for b in range(group.bit_length() - 1)]
    pl.when(k > 0)(lambda: signal(barrier, {"tm": jnp.maximum(k - 1, 0)}))
    pl.when(k < top)(lambda: signal(barrier, {"tm": jnp.minimum(k + 1, top)}))
    for d in bits:
        signal(barrier, {"par": flipped(d) * 2 + core})
    signal(barrier, {"par": partner})

    history_load = pltpu.make_async_copy(h_ref, xbuf.at[pl.ds(0, block_len)], load_s.at[0])
    kernel_loads = [
        pltpu.make_async_copy(
            k_ref.at[block_len - 1 - j], kflat.at[:, pl.ds(j * params, params)], load_s.at[1]
        )
        for j in range(block_len)
    ]
    first_pieces = []
    for s in range(steps):
        place = xbuf.at[pl.ds(block_len * (s + 1), piece)]
        first_pieces.append(pltpu.make_async_copy(a_ref.at[s], place, load_s.at[2 + s]))
    place = xbuf.at[pl.ds(2 * block_len + piece, piece)]
    own_piece = pltpu.make_async_copy(a_ref.at[0], place, load_s.at[2])

    arrival_load = pltpu.make_async_copy(a_ref, abuf, load_s.at[2 + steps])

    history_load.start()
    arrival_load.start()
    for copy in kernel_loads:
        copy.start()

    @pl.when(k == 0)
    def _():
        for copy in first_pieces:
            copy.start()

    pl.when(k == 1)(own_piece.start)

    wide = 2 * piece
    @pl.when((k > 0) & (k < top - 1))
    def _():
        kext[:, pl.ds(0, piece * params)] = jnp.zeros((sensors, piece * params), BF16)

    @pl.when((k > 1) & (k < top))
    def _():
        tail = xbuf.at[pl.ds(block_len + last * piece, piece)]
        tail[...] = jnp.zeros(tail.shape, BF16)

    @pl.when(k == top)
    def _():
        xbuf[pl.ds(block_len + split * piece, 1)] = jnp.zeros((1, params, fields), BF16)

    zext[pl.ds(0, wide - 1 + piece)] = jnp.zeros((wide - 1 + piece, params, fields), BF16)

    around = (k < top).astype(jnp.int32) + (k > 0).astype(jnp.int32)
    pl.semaphore_wait(barrier, 1 + len(bits) + around)

    def slot(c):
        return xbuf.at[pl.ds(block_len + c * piece, piece)]

    up, down = {"tm": jnp.minimum(k + 1, top)}, {"tm": jnp.maximum(k - 1, 0)}
    sends_up = k < top
    forwards = (k > 0) & (k < top)

    history_copies = [
        remote(xbuf.at[pl.ds(i * piece, piece)], slot(i), hist_s, x_r.at[i], up)
        for i in range(tm_count)
    ]

    def parts(c):
        if c == split:
            return [(0, half, c), (half, piece - half, pieces)]
        return [(0, piece, c)]

    def into(c, src, send, where):
        return [
            remote(
                src.at[pl.ds(first, count)],
                xbuf.at[pl.ds(block_len + c * piece + first, count)],
                send, x_r.at[sem], where,
            )
            for first, count, sem in parts(c)
        ]

    forward_copies = [
        into(i + tm_count, slot(i), fwd_s, up) for i in range(tm_count - 1)
    ]

    def arrivals_from(step, s, target, c):
        copies = into(c, abuf.at[s], arr_s.at[s], {"tm": target})
        return [(k == step, copy) for copy in copies]

    near_copies = arrivals_from(0, 0, 1, tm_count)
    near_copies += arrivals_from(1, 0, 0, 1) + arrivals_from(1, 1, 0, tm_count + 1)
    near_copies += arrivals_from(2, 0, 1, tm_count + 2)
    far_copies, late_copies = [], []
    for i in range(2, tm_count):
        if i > 2:
            far_copies += arrivals_from(i, 0, (i + 1) % 2, i if i % 2 else tm_count + i)
        late_copies += arrivals_from(i, 1, 0, tm_count + i)
    evens, odds = range(2, tm_count, 2), range(3, tm_count, 2)
    relay_copies = {
        i: remote(slot(tm_count + i), slot(i), relay_s, x_r.at[i], {"tm": 0}) for i in evens
    } | {
        i: remote(slot(i), slot(tm_count + i), relay_s, x_r.at[tm_count + i], {"tm": 1})
        for i in odds
    }
    def ext_copy(n, begin=0, count=piece):
        first = (block_len - (n + 1) * piece + begin) * params
        source = kflat.at[:, pl.ds(first, count * params)]
        place = kext.at[:, pl.ds(((1 - n) * piece + begin) * params, count * params)]
        return remote(source, place, ext_s, ext_r.at[n], down)

    sends_ext = k > 1

    history_load.wait()

    @pl.when(sends_up)
    def _():
        for copy in history_copies:
            copy.start()

    arrival_load.wait()
    for condition, copy in near_copies:
        pl.when(condition)(copy.start)

    pltpu.make_async_copy(kflat, kflat, load_s.at[1]).wait()
    pl.when(k == top)(ext_copy(1, 0, 1).start)
    pl.when(k > 0)(lambda: pl.semaphore_wait(ready, 1))
    pl.when(sends_up)(lambda: signal(ready, up))

    for condition, copy in far_copies:
        pl.when(condition)(copy.start)

    if bits[1:]:
        signal(near.at[0], {"par": flipped(1) * 2 + core})

    pl.when(sends_ext)(ext_copy(0).start)
    pl.when(k == top)(ext_copy(1, 1, piece - 1).start)

    @pl.when(k == 0)
    def _():
        for copy in first_pieces:
            copy.wait()

    pl.when(k == 1)(own_piece.wait)

    for n, d in enumerate(bits[:-1]):
        pl.semaphore_wait(near.at[n], 1)
        if n + 1 < len(bits) - 1:
            signal(near.at[n + 1], {"par": flipped(bits[n + 1]) * 2 + core})

    def taken(unit):
        c = split if unit == pieces else unit
        first, count = [(f, n) for f, n, sem in parts(c) if sem == unit][0]
        place = xbuf.at[pl.ds(block_len + c * piece + first, count)]
        return remote(place, place, hist_s, x_r.at[unit], up)

    def receive(unit):
        c = split if unit == pieces else unit
        i = c % tm_count
        waits = k >= 0
        if i == c:
            waits = (k != 0) if c == 0 or c in odds else waits
        elif i < 2:
            waits = k != i
        elif i % 2 == 0:
            waits = k != 1
        if c == last:
            waits = waits & (k < 2)
        if c == split:
            waits = waits & (k < top)
        pl.when(waits)(taken(unit).wait_recv)

    def relay():
        @pl.when(k == 1)
        def _():
            for i in evens:
                for _, _, unit in parts(tm_count + i):
                    taken(unit).wait_recv()
                relay_copies[i].start()

        @pl.when(k == 0)
        def _():
            for i in odds:
                taken(i).wait_recv()
                relay_copies[i].start()

    def late():
        for condition, copy in late_copies:
            pl.when(condition)(copy.start)

    def span(c):
        return pl.ds(*spans[c])

    def flat_span(c):
        first, count = spans[c]
        return pl.ds(first * rows, count * rows)

    def core_copy(c):
        return remote(
            buf0.at[1 - core, :, span(c)], rcv0.at[:, span(c)], s0, r0.at[c],
            {"par": partner},
        )

    def chip_copy(c, d):
        target = flipped(d)
        return remote(
            mid.at[target, span(c)], mrcv.at[d - 1, span(c)], ms, mr.at[c],
            {"par": target * 2 + core},
        )

    def tm_copy(c, d):
        target = lax.rem(k + d, tm_count)
        place = flat_span(c)
        return remote(
            zbuf.at[target, place], zrcv.at[d - 1, place], zs, zr.at[tm_sem(c)],
            {"tm": target},
        )

    def tm_sem(c):
        return max(c - (split - 2), 0)

    def product(r, low, high):
        count = (high - low) * params
        left = xbuf[pl.ds(r + 1 + low, high - low)].reshape(count, fields)
        right = xbuf[pl.ds(r + 2 + low, high - low)].reshape(count, fields)
        both = jnp.concatenate([left, right], 1)
        lags = kflat[:, low * params : high * params]
        return jnp.dot(lags, both, preferred_element_type=F32)

    def hand_over(r, total):
        for side in range(2):
            mine = total[:, side * fields : (side + 1) * fields]
            moved = jnp.concatenate([mine[o * rows : (o + 1) * rows] for o in order], 0)
            moved = moved.astype(BF16)
            for n in range(2 * group):
                buf0[n // group, n % group, r + side] = moved[n * share : (n + 1) * share]

    def compute(c):
        receive(c)
        if c < tm_count - 1:

            @pl.when(forwards & (k < top - 1) if c == tm_count - 2 else forwards)
            def _():
                for copy in forward_copies[c]:
                    copy.start()

        first, count = spans[c]
        for r in range(first, first + count, 2):
            hand_over(r, product(r, 0, block_len))
        core_copy(c).start()

    begin = (split - 1) * piece
    last_rows = list(enumerate(range(begin, steps * block_len, 2)))
    latest = [(n, r) for n, r in last_rows if r >= split * piece]

    def bound(r, c):
        return block_len + c * piece - r - 2

    def early():
        for n, r in last_rows:
            acc[n] = product(r, 0, bound(r, split - 1))

    def extra():
        rest = 2 * block_len - wide
        zext[pl.ds(wide - 1 + piece, piece)] = xbuf[pl.ds(rest + piece, piece)]

        @pl.when(k == top - 1)
        def _():
            zext[pl.ds(wide - 1, piece)] = xbuf[pl.ds(rest, piece)]
            ext_copy(1).wait_recv()

        ext_copy(0).wait_recv()
        left = zext[pl.ds(wide - 2, wide)].reshape(wide * params, fields)
        right = zext[pl.ds(wide - 1, wide)].reshape(wide * params, fields)
        both = jnp.concatenate([left, right], 1)
        for n, r in latest:
            count = (r + 2 - split * piece) * params
            lags = kext[:, wide * params - count :]
            acc[n] = acc[n] + jnp.dot(lags, both[:count], preferred_element_type=F32)

    def middle():
        for n, r in latest:
            acc[n] = acc[n] + product(r, bound(r, split - 1), bound(r, split))

    def final(c):
        receive((split - 1, split, pieces, last)[c - split + 1])
        first, count = spans[c]
        for r in range(first, first + count, 2):
            n = (r - begin) // 2
            hand_over(r, acc[n] + product(r, bound(r, min(c, split)), block_len))
        core_copy(c).start()

    def close(c):
        first, count = spans[c]
        for r in range(first, first + count, 2):
            n = (r - begin) // 2
            hand_over(r, acc[n] + product(r, bound(r, split - 1), bound(r, split) + 1))
        core_copy(c).start()

    def across(c):
        core_copy(c).wait_recv()
        total = buf0[core, :, span(c)].astype(F32) + rcv0[:, span(c)].astype(F32)
        mid[:, span(c)] = total.astype(BF16)
        pl.when(chip == 1)(chip_copy(c, 1).start)
        for d in flips:
            if d == 1:
                pl.when(chip != 1)(chip_copy(c, d).start)
            else:
                chip_copy(c, d).start()

    def goes_up(d):
        return k + d < tm_count

    def spread(c):
        total = mid[chip, span(c)].astype(F32)
        place = mrcv.at[:, span(c)]
        remote(place, place, ms, mr.at[c], {"par": par}).wait_recv()
        for d in range(1, group):
            total = total + mrcv[d - 1, span(c)].astype(F32)
        for t in range(tm_count):
            mine = [total[g, t * rows : (t + 1) * rows] for g in range(spans[c][1])]
            zbuf[t, flat_span(c)] = jnp.concatenate(mine, 0).astype(BF16)
        for d in range(1, tm_count):
            pl.when(jnp.logical_not(goes_up(d)))(tm_copy(c, d).start)

    def rise(c):
        for d in range(1, tm_count):
            pl.when(goes_up(d))(tm_copy(c, d).start)

    def finish(c):
        place = flat_span(c)
        total = zbuf[k, place].astype(F32)
        if tm_sem(c):
            taken_parts = zrcv.at[:, place]
        else:
            taken_parts = zrcv.at[:, pl.ds(0, (split - 1) * piece * rows)]
        if tm_sem(c) or c == 0:
            remote(taken_parts, taken_parts, zs, zr.at[tm_sem(c)], {"tm": k}).wait_recv()
        for d in range(1, tm_count):
            total = total + zrcv[d - 1, place].astype(F32)
        first, count = spans[c]
        total = total.reshape(count, rows, fields).astype(out_ref.dtype)
        first = first % block_len
        out_ref[spans[c][0] // block_len, first : first + count] = total

    def across_on(which, c):
        pl.when(core == which)(lambda: across(c))

    def run(plan):
        for stage, *c in plan:
            stage(*c)

    ends = [(across, split + 1), (across, split + 2), (spread, split - 2)]
    ends += [(rise, c) for c in range(split - 1)]
    ends += [(spread, split - 1), (rise, split - 1)]
    for c in range(split, chunks):
        ends += [(spread, c), (rise, c)]

    @pl.when(k == 0)
    def _():
        plan = [(compute, 0), (across, 0), (compute, 1), (relay,), (across, 1), (spread, 0)]
        for c in range(2, split - 1):
            plan.append((compute, c))
            if c > 2:
                plan.append((across, c - 1))
            if c > 3:
                plan.append((spread, c - 3))
        plan += [(early,), (final, split - 1), (across, split - 2), (spread, split - 4)]
        plan += [(across, split - 1), (spread, split - 3), (middle,)]
        plan += [(final, c) for c in range(split, chunks)]
        run(plan + [(across, split)] + ends)

    def paced(tail):
        plan = []
        for c in range(split - 1):
            plan.append((compute, c))
            if c == split - 2:
                plan += [(across_on, 0, c), (early,)]
            else:
                plan.append((across, c))
            if c == 0:
                plan.append((relay,))
            if c == 2:
                plan.append((late,))
            if 2 <= c < split - 2:
                plan.append((spread, c - 2))
        run(plan + [(spread, split - 4)] + tail + ends)

    @pl.when(forwards)
    def _():
        tail = [(extra,), (final, split - 1), (across_on, 1, split - 2)]
        tail += [(across_on, 0, split - 1), (middle,), (final, split), (across_on, 0, split)]
        tail += [(final, split + 1), (final, split + 2), (across_on, 1, split - 1)]
        paced(tail + [(across_on, 1, split), (spread, split - 3)])

    @pl.when(k == top)
    def _():
        tail = [(final, split - 1), (across_on, 0, split - 1), (close, split)]
        tail += [(across_on, 0, split), (across_on, 1, split - 2), (close, split + 1)]
        tail += [(close, split + 2), (across_on, 1, split - 1), (across_on, 1, split)]
        paced(tail + [(spread, split - 3)])

    run([(finish, c) for c in range(chunks)])

    def sent(place, sem):
        return remote(place, place, sem, x_r.at[0], up).wait_send

    pl.when(sends_up)(sent(xbuf.at[pl.ds(0, block_len)], hist_s))
    pl.when(forwards)(sent(xbuf.at[pl.ds(0, block_len - wide)], fwd_s))
    pl.when(forwards & (k < top - 1))(sent(xbuf.at[pl.ds(0, piece)], fwd_s))
    sent(abuf.at[0], arr_s.at[0])()
    pl.when(k > 0)(sent(abuf.at[1], arr_s.at[1]))
    for step, those in ((1, evens), (0, odds)):
        if those:
            pl.when(k == step)(sent(xbuf.at[pl.ds(0, len(those) * piece)], relay_s))
    pl.when(sends_ext)(ext_copy(0).wait_send)
    pl.when(k == top)(ext_copy(1).wait_send)
    sent(rcv0, s0)()
    sent(mrcv, ms)()
    sent(zrcv, zs)()


def fused(tm_count, group, kernel, history, arrivals):
    block_len, sensors, params = kernel.shape
    fields = history.shape[2]
    steps = arrivals.shape[0]
    piece = block_len // tm_count
    pieces = steps * tm_count
    outputs = steps * block_len
    share = sensors // (2 * group)
    rows = share // tm_count
    dma = pltpu.SemaphoreType.DMA
    scratch = [
        pltpu.VMEM((sensors, block_len * params), BF16),
        pltpu.VMEM((sensors, 2 * piece * params), BF16),
        pltpu.VMEM(((steps + 1) * block_len, params, fields), BF16),
        pltpu.VMEM((steps, piece, params, fields), BF16),
        pltpu.VMEM((4 * piece - 1, params, fields), BF16),
        pltpu.VMEM((piece + piece // 2, sensors, 2 * fields), F32),
        pltpu.VMEM((2, group, outputs, share, fields), BF16),
        pltpu.VMEM((group, outputs, share, fields), BF16),
        pltpu.VMEM((group, outputs, share, fields), BF16),
        pltpu.VMEM((group - 1, outputs, share, fields), BF16),
        pltpu.VMEM((tm_count, outputs * rows, fields), BF16),
        pltpu.VMEM((tm_count - 1, outputs * rows, fields), BF16),
        dma((3 + steps,)),
        dma(()),
        dma(()),
        dma((2,)),
        dma(()),
        dma(()),
        dma((pieces + 1,)),
        dma((2,)),
        dma(()),
        dma((pieces + 1,)),
        dma(()),
        dma((pieces + 1,)),
        dma(()),
        dma((5,)),
        pltpu.SemaphoreType.REGULAR,
        pltpu.SemaphoreType.REGULAR((max(group.bit_length() - 2, 1),)),
    ]
    out_bytes = steps * block_len * rows * fields * 2
    return pl.pallas_call(
        functools.partial(kernel_body, tm_count, group),
        out_shape=pltpu.VMEM((steps, block_len, rows, fields), BF16),
        in_specs=[pl.BlockSpec(memory_space=pltpu.HBM)] * 3,
        out_specs=pl.BlockSpec(memory_space=pltpu.VMEM),
        scratch_shapes=scratch,
        compiler_params=pltpu.CompilerParams(
            collective_id=0, has_side_effects=True, vmem_limit_bytes=VMEM_BYTES - 2 * out_bytes
        ),
    )(kernel, history, arrivals)


def plain(tm_count, kernel, history, arrivals):
    block_len, sensors, params = kernel.shape
    fields = history.shape[2]
    steps = arrivals.shape[0]
    incoming = lax.all_gather(arrivals, "tm", axis=1, tiled=True)
    position = lax.axis_index("tm")
    pairs = [(i, i + 1) for i in range(tm_count - 1)]
    blocks = [history]
    for s in range(steps):
        shifted = lax.ppermute(blocks[-1], "tm", pairs)
        blocks.append(jnp.where(position == 0, incoming[s], shifted))
    window = jnp.concatenate(blocks, 0)
    flat = kernel[::-1].transpose(1, 0, 2).reshape(sensors, block_len * params)

    def one(first):
        part = lax.dynamic_slice_in_dim(window, first, block_len, 0)
        part = part.reshape(block_len * params, fields)
        return jnp.dot(flat, part, preferred_element_type=F32)

    partial = lax.map(one, jnp.arange(steps * block_len, dtype=jnp.int32) + 1)
    partial = partial.reshape(steps, block_len, sensors, fields)
    total = lax.psum_scatter(partial, ("tm", "par"), scatter_dimension=2, tiled=True)
    return total.astype(BF16)


def solution(mesh):
    tm_count, par_count = mesh.shape["tm"], mesh.shape["par"]

    def per_device(kernel, history, arrivals):
        rows = kernel.shape[1] // (tm_count * par_count)
        piece = kernel.shape[0] // tm_count
        fits = rows % 8 == 0 and piece % 4 == 0 and tm_count > 3 and arrivals.shape[0] == 2
        if fits and par_count > 2 and par_count.bit_count() == 1:
            return fused(tm_count, par_count // 2, kernel, history, arrivals)
        return plain(tm_count, kernel, history, arrivals)

    in_specs = (P("tm", None, "par"), P("tm", "par", None), P(None, "tm", "par", None))
    out_specs = P(None, None, ("tm", "par"), None)
    return jax.shard_map(
        per_device, mesh=mesh, in_specs=in_specs, out_specs=out_specs, check_vma=False
    )
```
